32 devices in a mesh: grp: 2 (over core), ex: 16 (over z, y, x).
Axes of the slice: x: 2, y: 2, z: 4, core: 2. Of those that a mesh axis runs over, the one named last changes fastest.
Arguments:
- tokens: bfloat16 [8192, 1024], P(('grp', 'ex')), may hold values from -6 to 6
- expert_ids: int32 [8192], P(('grp', 'ex')), may hold values from 0 to 15, as said below
- slot_ids: int32 [8192], P(('grp', 'ex')), may hold values from 0 to 31, as said below
- centroids: bfloat16 [16, 1024], replicated, may hold values from -0.1875 to 0.1875
- w_in: bfloat16 [16, 1024, 4096], P('ex', None, 'grp'), may hold values from -0.1875 to 0.1875
- w_out: bfloat16 [16, 4096, 1024], P('ex', 'grp'), may hold values from -0.09375 to 0.09375
Outputs:
- combined: bfloat16 [8192, 1024], P(('grp', 'ex'))
The draws below stay inside these ranges and needn't reach their ends.
Inputs may be any that keep to these rules, and one draw needn't show every extreme that they name: `expert_ids`: within each device's 256 rows, at most 32 rows name one expert; in every device some expert is named by exactly 32 rows, and in each group of 16 devices along ex one expert is named by 32 rows on every device of the group. `slot_ids`: rows of one device that name the same expert have distinct slots.
All inputs are finite; a program needn't handle non-finite values.
Results may differ from the reference program's by a relative error of at most 0.0035.
Values may be sent and summed in bfloat16 or wider, within the bound.
A program may use at most 128 MiB of HBM per device.

```python
import jax
import jax.numpy as jnp
from jax import lax

D = 1024
FF = 4096
TOK_DEV = 256
EXPERTS = 16
TOKENS = 8192
CAP = 32


def assignment(key):
    base_key = jax.random.fold_in(key, 11)
    group_count = TOKENS // (TOK_DEV * EXPERTS)
    hot_experts = jax.random.randint(jax.random.fold_in(base_key, 1), (group_count,), 0, EXPERTS)
    block_keys = jax.random.split(jax.random.fold_in(base_key, 2), TOKENS // TOK_DEV)
    hot_list = jnp.repeat(hot_experts, EXPERTS)

    def one_block(block_key, hot_one):
        key_full, key_perm, key_rows = jax.random.split(block_key, 3)
        favoured = jax.random.randint(key_full, (), 0, EXPERTS)
        shuffled = jax.random.permutation(key_perm, EXPERTS * CAP).astype(jnp.int32)
        owner = shuffled // CAP
        classes = jnp.where(owner == hot_one, 0, jnp.where(owner == favoured, 1, 2)).astype(jnp.int32)
        ordering = jnp.argsort(classes * (EXPERTS * CAP) + jnp.arange(EXPERTS * CAP, dtype=jnp.int32))
        picked = shuffled[ordering][:TOK_DEV]
        picked = picked[jax.random.permutation(key_rows, TOK_DEV)]
        return (picked // CAP, picked % CAP)
    owners, places = jax.vmap(one_block)(block_keys, hot_list)
    return (owners.reshape(-1).astype(jnp.int32), places.reshape(-1).astype(jnp.int32))


def draw_expert_ids(key, part):
    return assignment(key)[0]


def draw_slot_ids(key, part):
    return assignment(key)[1]


def level_of(key, extent, shards, least, largest):
    def one(position, parts):
        draws = jax.random.uniform(jax.random.fold_in(jax.random.fold_in(key, 6), position), (parts,), jnp.float32, least / len(shards), largest / len(shards))
        return jnp.repeat(jnp.exp(draws), extent[position] // parts).reshape((-1,) + (1,) * (len(extent) - position - 1))

    gain = one(*shards[0])
    for cut in shards[1:]:
        gain = gain * one(*cut)
    return gain


def scatter_about(stream_key, dims, scale, reach, pieces=(), held_as=jnp.bfloat16):
    result = scale * jax.random.normal(stream_key, dims, jnp.float32)
    if pieces:
        result = result * level_of(stream_key, dims, pieces, -0.22, 0.18)
    return jnp.clip(result, -reach, reach).astype(held_as)


def setup_inputs(seed: int = 0) -> dict:
    keys = jax.random.split(jax.random.key(seed), 7)
    tokens = scatter_about(keys[0], (TOKENS, D), 1.0, 6.0, ((0, 32),))
    expert_ids = draw_expert_ids(jax.random.fold_in(keys[6], 71), 0)
    slot_ids = draw_slot_ids(jax.random.fold_in(keys[6], 71), 0)
    centroids = scatter_about(keys[3], (EXPERTS, D), D ** -0.5, 0.1875)
    w_in = scatter_about(keys[4], (EXPERTS, D, FF), D ** -0.5, 0.1875, ((0, 16), (2, 2)))
    w_out = scatter_about(keys[5], (EXPERTS, FF, D), FF ** -0.5, 0.09375, ((0, 16), (1, 2)))
    return {"tokens": tokens, "expert_ids": expert_ids, "slot_ids": slot_ids, "centroids": centroids, "w_in": w_in, "w_out": w_out}


def reference(tokens, expert_ids, slot_ids, centroids, w_in, w_out):
    block_count = TOKENS // TOK_DEV
    block_ids = jnp.arange(TOKENS, dtype=jnp.int32) // TOK_DEV
    buffer_rows = (expert_ids * (block_count * CAP) + block_ids * CAP + slot_ids).astype(jnp.int32)
    total_rows = EXPERTS * block_count * CAP
    buffer = jnp.zeros((total_rows, D), jnp.bfloat16).at[buffer_rows].set(tokens)
    buffer = buffer.reshape(EXPERTS, block_count * CAP, D)

    def expert(operands):
        rows_in, first, second = operands
        hidden = jnp.maximum(jnp.dot(rows_in, first, preferred_element_type=jnp.float32), 0.0).astype(jnp.bfloat16)
        return jnp.dot(hidden, second, preferred_element_type=jnp.float32).astype(jnp.bfloat16)

    results = lax.map(expert, (buffer, w_in, w_out)).reshape(total_rows, D)
    arrived = results[buffer_rows]
    scores = jnp.dot(tokens, centroids.T, preferred_element_type=jnp.float32)
    columns = jnp.arange(EXPERTS, dtype=jnp.int32)
    chosen = jnp.sum(jnp.where(columns[None, :] == expert_ids[:, None], scores, 0.0), axis=1)
    gating = jax.nn.sigmoid(chosen)
    return (tokens.astype(jnp.float32) + gating[:, None] * arrived.astype(jnp.float32)).astype(jnp.bfloat16)
```

```python
import functools

import jax
import jax.numpy as jnp
from jax import lax
from jax.experimental import pallas as pl
from jax.experimental.pallas import tpu as pltpu
from jax.sharding import PartitionSpec as P

MESH = pl.DeviceIdType.MESH
TILE = 1024
ORDER = (1, 3, 2, "home", 0)
FINISH = (1, 2, 0, 3)


def expert_kernel(
    n,
    cap,
    ids_ref,
    slots_ref,
    tokens_hbm,
    centroids_ref,
    w_in_ref,
    w_out_ref,
    out_ref,
    outgoing,
    received,
    result,
    returned,
    total,
    tokens_ref,
    place,
    columns,
    full_in,
    full_out,
    load_sem,
    share_send,
    share_recv,
    send_sem,
    recv_sem,
    back_send,
    back_recv,
):
    grp = lax.axis_index("grp")
    me = lax.axis_index("ex")
    half = n // 2
    side = me // half
    seat = me % half
    quarter = n // 4
    rows = quarter * cap
    tokens_here, width = tokens_ref.shape
    hidden = full_in.shape[2]

    def peer_to(slot):
        return ((side + slot // half) % 2) * half + (seat + slot % half) % half

    def peer_from(slot):
        return ((side + slot // half) % 2) * half + (seat + half - slot % half) % half

    def block(slot):
        start = slot * cap
        if not isinstance(slot, int):
            start = pl.multiple_of(start, cap)
        return pl.ds(start, cap)

    barrier = pltpu.get_barrier_semaphore()
    for slot in range(1, n):
        pl.semaphore_signal(
            barrier, inc=1, device_id={"ex": peer_to(slot)}, device_id_type=MESH
        )
    pl.semaphore_signal(barrier, inc=1, device_id={"grp": 1 - grp}, device_id_type=MESH)

    bring = pltpu.make_async_copy(tokens_hbm, tokens_ref, load_sem.at[2])
    bring.start()
    loads = [
        pltpu.make_async_copy(w_in_ref.at[0], full_in.at[0], load_sem.at[0]),
        pltpu.make_async_copy(w_out_ref.at[0], full_out.at[0], load_sem.at[1]),
    ]
    for load in loads:
        load.start()

    ids = ids_ref[...]
    high = (ids >= half).astype(jnp.int32)
    ahead = ids - high * half - seat
    ahead = jnp.where(ahead < 0, ahead + half, ahead)
    across = jnp.where(high == side, 0, 1)
    position = (across * half + ahead) * cap + slots_ref[...]
    slot_rows = lax.broadcasted_iota(jnp.int32, (n * cap, tokens_here), 0)
    spread = (slot_rows == position).astype(jnp.bfloat16)
    bring.wait()
    packed = jnp.dot(spread, tokens_ref[...], preferred_element_type=jnp.float32)
    packed = packed.astype(jnp.bfloat16)
    outgoing[...] = packed
    received[block(0), :] = packed[:cap]

    shares = [
        pltpu.make_async_remote_copy(
            src_ref=w_in_ref.at[0],
            dst_ref=full_in.at[1],
            send_sem=share_send.at[0],
            recv_sem=share_recv.at[0],
            device_id={"grp": 1 - grp},
            device_id_type=MESH,
        ),
        pltpu.make_async_remote_copy(
            src_ref=w_out_ref.at[0],
            dst_ref=full_out.at[1],
            send_sem=share_send.at[1],
            recv_sem=share_recv.at[1],
            device_id={"grp": 1 - grp},
            device_id_type=MESH,
        ),
    ]

    def dispatch(slot):
        return pltpu.make_async_remote_copy(
            src_ref=outgoing.at[block(slot), :],
            dst_ref=received.at[block(slot), :],
            send_sem=send_sem.at[slot],
            recv_sem=recv_sem.at[slot],
            device_id={"ex": peer_to(slot)},
            device_id_type=MESH,
        )

    def give_back(slot):
        return pltpu.make_async_remote_copy(
            src_ref=result.at[block(slot), :],
            dst_ref=returned.at[block(slot), :],
            send_sem=back_send.at[slot],
            recv_sem=back_recv.at[slot],
            device_id={"ex": peer_from(slot)},
            device_id_type=MESH,
        )

    pl.semaphore_wait(barrier, n)
    for step in reversed(range(half)):
        dispatch(half + step).start()
        if step > 0:
            dispatch(step).start()
    for share in shares:
        share.start()

    scores = lax.dot_general(
        centroids_ref[...],
        tokens_ref[...],
        (((1,), (1,)), ((), ())),
        preferred_element_type=jnp.float32,
    )
    experts = lax.broadcasted_iota(jnp.int32, scores.shape, 0)
    chosen = jnp.sum(jnp.where(experts == ids, scores, 0.0), axis=0, keepdims=True)
    gating = 1.0 / (1.0 + jnp.exp(-chosen))
    lines = lax.broadcasted_iota(jnp.int32, (128, tokens_here), 0)
    columns[...] = jnp.where(lines == 0, position.astype(jnp.float32), gating).T
    slot_columns = lax.broadcasted_iota(jnp.int32, (tokens_here, n * cap), 1)
    place[...] = (slot_columns == columns[:, 0:1].astype(jnp.int32)).astype(jnp.bfloat16)

    for load in loads:
        load.wait()
    for share in shares:
        share.wait_recv()

    @pl.loop(0, 4)
    def _(turn):
        chunk = 3 - (2 * turn) % 4 - turn // 2
        first = chunk * quarter

        @pl.loop(0, quarter)
        def _(k):
            @pl.when(first + k > 0)
            def _():
                dispatch(first + k).wait_recv()

        here = pl.ds(pl.multiple_of(chunk * rows, rows), rows)
        total[...] = jnp.zeros_like(total)

        @pl.loop(0, 2 * (hidden // TILE))
        def _(piece):
            part = piece // (hidden // TILE)
            cut = pl.ds(pl.multiple_of((piece % (hidden // TILE)) * TILE, TILE), TILE)
            middle = jnp.dot(
                received[here, :], full_in[part, :, cut], preferred_element_type=jnp.float32
            )
            middle = jnp.maximum(middle, 0.0).astype(jnp.bfloat16)
            total[...] += jnp.dot(
                middle, full_out[part, cut, :], preferred_element_type=jnp.float32
            )

        result[here, :] = total[...].astype(jnp.bfloat16)

        @pl.loop(0, quarter)
        def _(k):
            @pl.when(first + k > 0)
            def _():
                give_back(first + k).start()

            @pl.when(first + k == 0)
            def _():
                returned[block(0), :] = result[block(0), :]

    arrived = jnp.zeros((tokens_here, width), jnp.float32)
    for chunk in (1, 3, 0, 2):
        for slot in range(chunk * quarter, (chunk + 1) * quarter):
            if slot > 0:
                give_back(slot).wait_recv()
        here = pl.ds(chunk * rows, rows)
        arrived += jnp.dot(
            place[:, here], returned[here, :], preferred_element_type=jnp.float32
        )
    mixed = tokens_ref[...].astype(jnp.float32) + columns[:, 1:2] * arrived
    out_ref[...] = mixed.astype(jnp.bfloat16)

    @pl.loop(1, n)
    def _(slot):
        dispatch(slot).wait_send()
        give_back(slot).wait_send()

    for share in shares:
        share.wait_send()


def in_one_kernel(n, tokens, expert_ids, slot_ids, centroids, w_in, w_out):
    count, width = tokens.shape
    cap = 2 * count // n
    slots = n * cap
    rows = slots // 4
    hidden = w_in.shape[2]
    vmem = pl.BlockSpec(memory_space=pltpu.VMEM)
    hbm = pl.BlockSpec(memory_space=pl.ANY)
    sems = pltpu.SemaphoreType.DMA
    return pl.pallas_call(
        functools.partial(expert_kernel, n, cap),
        out_shape=pltpu.VMEM((count, width), jnp.bfloat16),
        in_specs=[vmem, vmem, hbm, vmem, hbm, hbm],
        out_specs=vmem,
        scratch_shapes=[
            pltpu.VMEM((slots, width), jnp.bfloat16),
            pltpu.VMEM((slots, width), jnp.bfloat16),
            pltpu.VMEM((slots, width), jnp.bfloat16),
            pltpu.VMEM((slots, width), jnp.bfloat16),
            pltpu.VMEM((rows, width), jnp.float32),
            pltpu.VMEM((count, width), jnp.bfloat16),
            pltpu.VMEM((count, slots), jnp.bfloat16),
            pltpu.VMEM((count, 128), jnp.float32),
            pltpu.VMEM((2, width, hidden), jnp.bfloat16),
            pltpu.VMEM((2, hidden, width), jnp.bfloat16),
            sems((3,)),
            sems((2,)),
            sems((2,)),
            sems((n,)),
            sems((n,)),
            sems((n,)),
            sems((n,)),
        ],
        compiler_params=pltpu.CompilerParams(
            collective_id=0, has_side_effects=True, vmem_limit_bytes=60 * 1024 * 1024
        ),
    )(
        expert_ids.reshape(1, count),
        slot_ids.reshape(1, count),
        tokens,
        centroids,
        w_in,
        w_out,
    )


def relay_kernel(
    n,
    cap,
    spare,
    ids_ref,
    slots_ref,
    tokens_hbm,
    centroids_ref,
    w_in_ref,
    w_out_ref,
    out_ref,
    spill_ref,
    outgoing,
    pouch,
    inbox,
    expanded,
    received,
    result,
    collected,
    returned,
    total,
    tokens_ref,
    place,
    columns,
    full_in,
    full_out,
    flag_out,
    flags_in,
    group_out,
    group_in,
    load_sem,
    share_send,
    share_recv,
    send_sem,
    recv_sem,
    back_send,
    back_recv,
    relay_send,
    relay_recv,
    relay_back_send,
    relay_back_recv,
    pouch_send,
    pouch_recv,
    flag_send,
    flag_recv,
):
    grp = lax.axis_index("grp")
    me = lax.axis_index("ex")
    half = n // 2
    base = cap // 2
    side = me // half
    seat = me % half
    mirror = (1 - side) * half + seat
    near_rows = half * cap
    far_rows = half * base
    direct_rows = near_rows + far_rows
    rows = near_rows // 2
    tokens_here, width = tokens_ref.shape
    hidden = full_in.shape[2]
    pieces = hidden // TILE

    def peer_to(slot):
        return ((side + slot // half) % 2) * half + (seat + slot % half) % half

    def peer_from(slot):
        return ((side + slot // half) % 2) * half + (seat + half - slot % half) % half

    def block(slot):
        if slot < half:
            return pl.ds(slot * cap, cap)
        return pl.ds(near_rows + (slot - half) * base, base)

    def extra(k, start=0):
        return pl.ds(start + k * base, base)

    def remote(src, dst, send, recv, where):
        return pltpu.make_async_remote_copy(
            src_ref=src,
            dst_ref=dst,
            send_sem=send,
            recv_sem=recv,
            device_id=where,
            device_id_type=MESH,
        )

    def dispatch(slot):
        return remote(
            outgoing.at[block(slot), :],
            received.at[block(slot), :],
            send_sem.at[slot],
            recv_sem.at[slot],
            {"ex": peer_to(slot)},
        )

    def give_back(slot):
        return remote(
            result.at[block(slot), :],
            returned.at[block(slot), :],
            back_send.at[slot],
            back_recv.at[slot],
            {"ex": peer_from(slot)},
        )

    def forward(k):
        return remote(
            expanded.at[extra(k), :],
            received.at[extra(k, direct_rows), :],
            relay_send.at[k],
            relay_recv.at[k],
            {"ex": peer_to(k)},
        )

    def give_relay(k):
        return remote(
            result.at[extra(k, direct_rows), :],
            collected.at[extra(k), :],
            relay_back_send.at[k],
            relay_back_recv.at[k],
            {"ex": peer_from(k)},
        )

    send_pouch = remote(pouch, inbox, pouch_send.at[0], pouch_recv.at[0], {"ex": mirror})
    back_pouch = remote(
        expanded.at[pl.ds(0, spare), :],
        returned.at[pl.ds(direct_rows, spare), :],
        pouch_send.at[1],
        pouch_recv.at[1],
        {"ex": mirror},
    )

    def send_flag(slot):
        return remote(
            flag_out, flags_in.at[slot], flag_send.at[slot], flag_recv.at[slot], {"ex": peer_to(slot)}
        )

    swap_flag = remote(group_out, group_in, flag_send.at[0], flag_recv.at[0], {"grp": 1 - grp})

    barrier = pltpu.get_barrier_semaphore()
    for slot in range(1, n):
        pl.semaphore_signal(
            barrier, inc=1, device_id={"ex": peer_to(slot)}, device_id_type=MESH
        )
    pl.semaphore_signal(barrier, inc=1, device_id={"grp": 1 - grp}, device_id_type=MESH)

    bring = pltpu.make_async_copy(tokens_hbm, tokens_ref, load_sem.at[2])
    bring.start()
    loads = [
        pltpu.make_async_copy(w_in_ref.at[0], full_in.at[0], load_sem.at[0]),
        pltpu.make_async_copy(w_out_ref.at[0], full_out.at[0], load_sem.at[1]),
    ]
    for load in loads:
        load.start()

    ids = ids_ref[...]
    slots = slots_ref[...]
    high = (ids >= half).astype(jnp.int32)
    ahead = ids - high * half - seat
    ahead = jnp.where(ahead < 0, ahead + half, ahead)
    across = high != side
    order = (ids * cap + slots).astype(jnp.float32)
    floor = (ids * cap).astype(jnp.float32)
    columns[...] = jnp.broadcast_to(order, (128, tokens_here)).T
    order_column = columns[:, 0:1]
    before = jnp.logical_and(order_column >= floor, order_column < order)
    rank = jnp.sum(jnp.where(before, 1.0, 0.0), axis=0, keepdims=True)
    rank = rank.astype(jnp.int32)
    late = jnp.logical_and(across, rank >= base)
    lines = lax.broadcasted_iota(jnp.int32, (tokens_here, tokens_here), 0)
    lanes = lax.broadcasted_iota(jnp.int32, (tokens_here, tokens_here), 1)
    earlier = (lines < lanes).astype(jnp.bfloat16)
    marks = jnp.broadcast_to(jnp.where(late, 1.0, 0.0), (16, tokens_here)).astype(jnp.bfloat16)
    queue = jnp.dot(marks, earlier, preferred_element_type=jnp.float32)[0:1, :]
    queue = queue.astype(jnp.int32)
    position = jnp.where(
        across,
        jnp.where(late, direct_rows + queue, near_rows + ahead * base + rank),
        ahead * cap + slots,
    )
    spill = jnp.max(jnp.where(late, queue + 1, 0), axis=1, keepdims=True) > spare
    flag_out[...] = jnp.broadcast_to(jnp.where(spill, 1.0, 0.0), flag_out.shape)
    flags_in[0] = flag_out[...]

    slot_rows = lax.broadcasted_iota(jnp.int32, (direct_rows + spare, tokens_here), 0)
    hits = slot_rows == position
    spread = hits.astype(jnp.bfloat16)
    target = (ahead * base + rank - base + 1).astype(jnp.float32)
    aim = jnp.sum(jnp.where(hits[direct_rows:], target, 0.0), axis=1, keepdims=True)
    wide = lax.broadcasted_iota(jnp.int32, (spare, 128), 1).astype(jnp.float32)
    pouch[:, width:] = (wide == aim - 1.0).astype(jnp.bfloat16)
    bring.wait()
    packed = jnp.dot(spread, tokens_ref[...], preferred_element_type=jnp.float32)
    packed = packed.astype(jnp.bfloat16)
    outgoing[...] = packed[:direct_rows]
    pouch[:, :width] = packed[direct_rows:]
    received[block(0), :] = packed[:cap]

    shares = [
        remote(
            w_in_ref.at[0],
            full_in.at[1],
            share_send.at[0],
            share_recv.at[0],
            {"grp": 1 - grp},
        ),
        remote(
            w_out_ref.at[0],
            full_out.at[1],
            share_send.at[1],
            share_recv.at[1],
            {"grp": 1 - grp},
        ),
    ]

    pl.semaphore_wait(barrier, n)
    send_pouch.start()
    for step in reversed(range(half)):
        dispatch(half + step).start()
        if step > 0:
            dispatch(step).start()
    for share in shares:
        share.start()
    for slot in range(1, n):
        send_flag(slot).start()

    scores = lax.dot_general(
        centroids_ref[...],
        tokens_ref[...],
        (((1,), (1,)), ((), ())),
        preferred_element_type=jnp.float32,
    )
    experts = lax.broadcasted_iota(jnp.int32, scores.shape, 0)
    chosen = jnp.sum(jnp.where(experts == ids, scores, 0.0), axis=0, keepdims=True)
    gating = 1.0 / (1.0 + jnp.exp(-chosen))
    which = lax.broadcasted_iota(jnp.int32, (128, tokens_here), 0)
    columns[...] = jnp.where(which == 0, position.astype(jnp.float32), gating).T
    slot_columns = lax.broadcasted_iota(jnp.int32, (tokens_here, direct_rows + spare), 1)
    place[...] = (slot_columns == columns[:, 0:1].astype(jnp.int32)).astype(jnp.bfloat16)

    def relay_out():
        send_pouch.wait_recv()
        opened = lax.dot_general(
            inbox[:, width:],
            inbox[:, :width],
            (((0,), (0,)), ((), ())),
            preferred_element_type=jnp.float32,
        )
        opened = opened[:far_rows].astype(jnp.bfloat16)
        expanded[...] = opened
        received[extra(0, direct_rows), :] = opened[:base]
        for k in range(1, half):
            forward(k).start()

    def relay_home():
        for k in range(1, half):
            give_relay(k).wait_recv()
            forward(k).wait_send()
        closed = jnp.dot(
            inbox[:, width : width + far_rows],
            collected[...],
            preferred_element_type=jnp.float32,
        )
        expanded[0:spare, :] = closed.astype(jnp.bfloat16)
        back_pouch.start()

    def multiply(here, part):
        @pl.loop(0, pieces)
        def _(piece):
            cut = pl.ds(pl.multiple_of(piece * TILE, TILE), TILE)
            middle = jnp.dot(
                received[here, :], full_in[part, :, cut], preferred_element_type=jnp.float32
            )
            middle = jnp.maximum(middle, 0.0).astype(jnp.bfloat16)
            total[...] += jnp.dot(
                middle, full_out[part, cut, :], preferred_element_type=jnp.float32
            )

    ready = []

    def chunk(which):
        here = pl.ds(which * rows, rows)
        if which == 3:
            for k in range(1, half):
                forward(k).wait_recv()
        else:
            first = which * half // 2 if which < 2 else half
            count = half // 2 if which < 2 else half
            for slot in range(first, first + count):
                if slot > 0:
                    dispatch(slot).wait_recv()
        total[...] = jnp.zeros_like(total)
        if not ready:
            for load in loads:
                load.wait()
        multiply(here, 0)
        if not ready:
            for share in shares:
                share.wait_recv()
            ready.append(True)
        multiply(here, 1)
        done = total[...].astype(jnp.bfloat16)
        result[here, :] = done
        if which == 3:
            collected[extra(0), :] = done[:base]
            for k in range(1, half):
                give_relay(k).start()
        else:
            for slot in range(first, first + count):
                if slot > 0:
                    give_back(slot).start()
                else:
                    returned[block(0), :] = done[:cap]

    relay_out()
    for which in ORDER:
        if which == "home":
            relay_home()
        else:
            chunk(which)

    for slot in range(1, n):
        send_flag(slot).wait_recv()
    group = jnp.max(flags_in[...], axis=0)
    group_out[...] = group
    for slot in range(1, n):
        send_flag(slot).wait_send()
    swap_flag.start()

    arrived = jnp.zeros((tokens_here, width), jnp.float32)
    for which in FINISH:
        if which == 3:
            here = pl.ds(direct_rows, spare)
            back_pouch.wait_recv()
        else:
            here = pl.ds(which * rows, rows)
            first = which * half // 2 if which < 2 else half
            count = half // 2 if which < 2 else half
            for slot in range(first, first + count):
                if slot > 0:
                    give_back(slot).wait_recv()
        arrived += jnp.dot(
            place[:, here], returned[here, :], preferred_element_type=jnp.float32
        )
    mixed = tokens_ref[...].astype(jnp.float32) + columns[:, 1:2] * arrived
    out_ref[...] = mixed.astype(jnp.bfloat16)

    swap_flag.wait_recv()
    spill_ref[0, 0] = jnp.max(jnp.maximum(group_out[...], group_in[...])).astype(jnp.int32)

    swap_flag.wait_send()
    send_pouch.wait_send()
    back_pouch.wait_send()
    for k in range(1, half):
        give_relay(k).wait_send()
    for slot in range(1, n):
        dispatch(slot).wait_send()
        give_back(slot).wait_send()
    for share in shares:
        share.wait_send()


def with_relay(n, tokens, expert_ids, slot_ids, centroids, w_in, w_out):
    count, width = tokens.shape
    cap = 2 * count // n
    half = n // 2
    base = cap // 2
    spare = cap + cap // 2
    direct = half * (cap + base)
    hidden = w_in.shape[2]
    vmem = pl.BlockSpec(memory_space=pltpu.VMEM)
    hbm = pl.BlockSpec(memory_space=pl.ANY)
    sems = pltpu.SemaphoreType.DMA
    bf16 = jnp.bfloat16
    out, spill = pl.pallas_call(
        functools.partial(relay_kernel, n, cap, spare),
        out_shape=[
            pltpu.VMEM((count, width), bf16),
            jax.ShapeDtypeStruct((1, 1), jnp.int32),
        ],
        in_specs=[vmem, vmem, hbm, vmem, hbm, hbm],
        out_specs=[vmem, pl.BlockSpec(memory_space=pltpu.SMEM)],
        scratch_shapes=[
            pltpu.VMEM((direct, width), bf16),
            pltpu.VMEM((spare, width + 128), bf16),
            pltpu.VMEM((spare, width + 128), bf16),
            pltpu.VMEM((half * base, width), bf16),
            pltpu.VMEM((n * cap, width), bf16),
            pltpu.VMEM((n * cap, width), bf16),
            pltpu.VMEM((half * base, width), bf16),
            pltpu.VMEM((direct + spare, width), bf16),
            pltpu.VMEM((half * cap // 2, width), jnp.float32),
            pltpu.VMEM((count, width), bf16),
            pltpu.VMEM((count, direct + spare), bf16),
            pltpu.VMEM((count, 128), jnp.float32),
            pltpu.VMEM((2, width, hidden), bf16),
            pltpu.VMEM((2, hidden, width), bf16),
            pltpu.VMEM((8, 128), jnp.float32),
            pltpu.VMEM((n, 8, 128), jnp.float32),
            pltpu.VMEM((8, 128), jnp.float32),
            pltpu.VMEM((8, 128), jnp.float32),
            sems((3,)),
            sems((2,)),
            sems((2,)),
            sems((n,)),
            sems((n,)),
            sems((n,)),
            sems((n,)),
            sems((half,)),
            sems((half,)),
            sems((half,)),
            sems((half,)),
            sems((2,)),
            sems((2,)),
            sems((n,)),
            sems((n,)),
        ],
        compiler_params=pltpu.CompilerParams(
            collective_id=1, has_side_effects=True, vmem_limit_bytes=60 * 1024 * 1024
        ),
    )(
        expert_ids.reshape(1, count),
        slot_ids.reshape(1, count),
        tokens,
        centroids,
        w_in,
        w_out,
    )
    return lax.cond(
        spill[0, 0] > 0,
        lambda: in_one_kernel(n, tokens, expert_ids, slot_ids, centroids, w_in, w_out),
        lambda: out,
    )


def in_plain_ops(tokens, expert_ids, slot_ids, centroids, w_in, w_out):
    experts = centroids.shape[0]
    count_rows = tokens.shape[0]
    model_width = tokens.shape[1]
    capacity = 2 * count_rows // experts
    buffer_rows = expert_ids * capacity + slot_ids
    outgoing = (
        jnp.zeros((experts * capacity, model_width), jnp.bfloat16).at[buffer_rows].set(tokens)
    )
    outgoing = outgoing.reshape(experts, capacity, model_width)
    scores = jnp.dot(tokens, centroids.T, preferred_element_type=jnp.float32)
    columns = jnp.arange(experts, dtype=jnp.int32)
    chosen = jnp.sum(jnp.where(columns[None, :] == expert_ids[:, None], scores, 0.0), axis=1)
    gating = jax.nn.sigmoid(chosen)
    full_in, full_out = (
        lax.all_gather(w_in, "grp", axis=2, tiled=True),
        lax.all_gather(w_out, "grp", axis=1, tiled=True),
    )
    received = lax.all_to_all(outgoing, "ex", split_axis=0, concat_axis=0, tiled=True)
    flat_rows = received.reshape(-1, model_width)
    hidden = jnp.maximum(
        jnp.dot(flat_rows, full_in[0], preferred_element_type=jnp.float32), 0.0
    ).astype(jnp.bfloat16)
    result = jnp.dot(hidden, full_out[0], preferred_element_type=jnp.float32)
    returned = lax.all_to_all(
        result.astype(jnp.bfloat16).reshape(received.shape),
        "ex",
        split_axis=0,
        concat_axis=0,
        tiled=True,
    )
    arrived = returned.reshape(-1, model_width)[buffer_rows]
    mixed_rows = tokens.astype(jnp.float32) + gating[:, None] * arrived.astype(jnp.float32)
    return mixed_rows.astype(jnp.bfloat16)


def solution(mesh):
    n = mesh.shape["ex"]

    def on_device(tokens, expert_ids, slot_ids, centroids, w_in, w_out):
        capacity = 2 * tokens.shape[0] // n
        lanes_needed = (n // 2) * (capacity // 2)
        if mesh.shape["grp"] == 2 and n % 4 == 0 and capacity % 32 == 0 and lanes_needed <= 128:
            return with_relay(n, tokens, expert_ids, slot_ids, centroids, w_in, w_out)
        if mesh.shape["grp"] == 2 and n % 4 == 0 and capacity % 16 == 0:
            return in_one_kernel(n, tokens, expert_ids, slot_ids, centroids, w_in, w_out)
        return in_plain_ops(tokens, expert_ids, slot_ids, centroids, w_in, w_out)

    in_specs = (
        P(("grp", "ex"), None),
        P(("grp", "ex")),
        P(("grp", "ex")),
        P(),
        P("ex", None, "grp"),
        P("ex", "grp", None),
    )
    out_specs = P(("grp", "ex"), None)
    return jax.shard_map(
        on_device, mesh=mesh, in_specs=in_specs, out_specs=out_specs, check_vma=False
    )
```

```python
import functools

import jax
import jax.numpy as jnp
from jax import lax
from jax.experimental import pallas as pl
from jax.experimental.pallas import tpu as pltpu
from jax.sharding import PartitionSpec as P

MESH = pl.DeviceIdType.MESH
TILE = 1024
PLAN = ('pouch', 1, 2, 3, 8, 'settle', 'most', 9, 10, 11, 4, 5, 6, 7, 'relay', 'all', 12, 13, 14, 15, 'flags', 'n0', 'fa', 'n1', 'relayed', 'share', 'fb', 'drain', 'home')
FINISH = ('n0', 'n1', 'spill', 'fa', 'fb', 'pouch')


def expert_kernel(
    n,
    cap,
    ids_ref,
    slots_ref,
    tokens_hbm,
    centroids_ref,
    w_in_ref,
    w_out_ref,
    out_ref,
    outgoing,
    received,
    result,
    returned,
    total,
    tokens_ref,
    place,
    columns,
    full_in,
    full_out,
    load_sem,
    share_send,
    share_recv,
    send_sem,
    recv_sem,
    back_send,
    back_recv,
):
    grp = lax.axis_index("grp")
    me = lax.axis_index("ex")
    half = n // 2
    side = me // half
    seat = me % half
    quarter = n // 4
    rows = quarter * cap
    tokens_here, width = tokens_ref.shape
    hidden = full_in.shape[2]

    def peer_to(slot):
        return ((side + slot // half) % 2) * half + (seat + slot % half) % half

    def peer_from(slot):
        return ((side + slot // half) % 2) * half + (seat + half - slot % half) % half

    def block(slot):
        start = slot * cap
        if not isinstance(slot, int):
            start = pl.multiple_of(start, cap)
        return pl.ds(start, cap)

    barrier = pltpu.get_barrier_semaphore()
    for slot in range(1, n):
        pl.semaphore_signal(
            barrier, inc=1, device_id={"ex": peer_to(slot)}, device_id_type=MESH
        )
    pl.semaphore_signal(barrier, inc=1, device_id={"grp": 1 - grp}, device_id_type=MESH)

    bring = pltpu.make_async_copy(tokens_hbm, tokens_ref, load_sem.at[2])
    bring.start()
    loads = [
        pltpu.make_async_copy(w_in_ref.at[0], full_in.at[0], load_sem.at[0]),
        pltpu.make_async_copy(w_out_ref.at[0], full_out.at[0], load_sem.at[1]),
    ]
    for load in loads:
        load.start()

    ids = ids_ref[...]
    high = (ids >= half).astype(jnp.int32)
    ahead = ids - high * half - seat
    ahead = jnp.where(ahead < 0, ahead + half, ahead)
    across = jnp.where(high == side, 0, 1)
    position = (across * half + ahead) * cap + slots_ref[...]
    slot_rows = lax.broadcasted_iota(jnp.int32, (n * cap, tokens_here), 0)
    spread = (slot_rows == position).astype(jnp.bfloat16)
    bring.wait()
    packed = jnp.dot(spread, tokens_ref[...], preferred_element_type=jnp.float32)
    packed = packed.astype(jnp.bfloat16)
    outgoing[...] = packed
    received[block(0), :] = packed[:cap]

    shares = [
        pltpu.make_async_remote_copy(
            src_ref=w_in_ref.at[0],
            dst_ref=full_in.at[1],
            send_sem=share_send.at[0],
            recv_sem=share_recv.at[0],
            device_id={"grp": 1 - grp},
            device_id_type=MESH,
        ),
        pltpu.make_async_remote_copy(
            src_ref=w_out_ref.at[0],
            dst_ref=full_out.at[1],
            send_sem=share_send.at[1],
            recv_sem=share_recv.at[1],
            device_id={"grp": 1 - grp},
            device_id_type=MESH,
        ),
    ]

    def dispatch(slot):
        return pltpu.make_async_remote_copy(
            src_ref=outgoing.at[block(slot), :],
            dst_ref=received.at[block(slot), :],
            send_sem=send_sem.at[slot],
            recv_sem=recv_sem.at[slot],
            device_id={"ex": peer_to(slot)},
            device_id_type=MESH,
        )

    def give_back(slot):
        return pltpu.make_async_remote_copy(
            src_ref=result.at[block(slot), :],
            dst_ref=returned.at[block(slot), :],
            send_sem=back_send.at[slot],
            recv_sem=back_recv.at[slot],
            device_id={"ex": peer_from(slot)},
            device_id_type=MESH,
        )

    pl.semaphore_wait(barrier, n)
    for step in reversed(range(half)):
        dispatch(half + step).start()
        if step > 0:
            dispatch(step).start()
    for share in shares:
        share.start()

    scores = lax.dot_general(
        centroids_ref[...],
        tokens_ref[...],
        (((1,), (1,)), ((), ())),
        preferred_element_type=jnp.float32,
    )
    experts = lax.broadcasted_iota(jnp.int32, scores.shape, 0)
    chosen = jnp.sum(jnp.where(experts == ids, scores, 0.0), axis=0, keepdims=True)
    gating = 1.0 / (1.0 + jnp.exp(-chosen))
    lines = lax.broadcasted_iota(jnp.int32, (128, tokens_here), 0)
    columns[...] = jnp.where(lines == 0, position.astype(jnp.float32), gating).T
    slot_columns = lax.broadcasted_iota(jnp.int32, (tokens_here, n * cap), 1)
    place[...] = (slot_columns == columns[:, 0:1].astype(jnp.int32)).astype(jnp.bfloat16)

    for load in loads:
        load.wait()
    for share in shares:
        share.wait_recv()

    @pl.loop(0, 4)
    def _(turn):
        chunk = 3 - (2 * turn) % 4 - turn // 2
        first = chunk * quarter

        @pl.loop(0, quarter)
        def _(k):
            @pl.when(first + k > 0)
            def _():
                dispatch(first + k).wait_recv()

        here = pl.ds(pl.multiple_of(chunk * rows, rows), rows)
        total[...] = jnp.zeros_like(total)

        @pl.loop(0, 2 * (hidden // TILE))
        def _(piece):
            part = piece // (hidden // TILE)
            cut = pl.ds(pl.multiple_of((piece % (hidden // TILE)) * TILE, TILE), TILE)
            middle = jnp.dot(
                received[here, :], full_in[part, :, cut], preferred_element_type=jnp.float32
            )
            middle = jnp.maximum(middle, 0.0).astype(jnp.bfloat16)
            total[...] += jnp.dot(
                middle, full_out[part, cut, :], preferred_element_type=jnp.float32
            )

        result[here, :] = total[...].astype(jnp.bfloat16)

        @pl.loop(0, quarter)
        def _(k):
            @pl.when(first + k > 0)
            def _():
                give_back(first + k).start()

            @pl.when(first + k == 0)
            def _():
                returned[block(0), :] = result[block(0), :]

    arrived = jnp.zeros((tokens_here, width), jnp.float32)
    for chunk in (1, 3, 0, 2):
        for slot in range(chunk * quarter, (chunk + 1) * quarter):
            if slot > 0:
                give_back(slot).wait_recv()
        here = pl.ds(chunk * rows, rows)
        arrived += jnp.dot(
            place[:, here], returned[here, :], preferred_element_type=jnp.float32
        )
    mixed = tokens_ref[...].astype(jnp.float32) + columns[:, 1:2] * arrived
    out_ref[...] = mixed.astype(jnp.bfloat16)

    @pl.loop(1, n)
    def _(slot):
        dispatch(slot).wait_send()
        give_back(slot).wait_send()

    for share in shares:
        share.wait_send()


def in_one_kernel(n, tokens, expert_ids, slot_ids, centroids, w_in, w_out):
    count, width = tokens.shape
    cap = 2 * count // n
    slots = n * cap
    rows = slots // 4
    hidden = w_in.shape[2]
    vmem = pl.BlockSpec(memory_space=pltpu.VMEM)
    hbm = pl.BlockSpec(memory_space=pl.ANY)
    sems = pltpu.SemaphoreType.DMA
    return pl.pallas_call(
        functools.partial(expert_kernel, n, cap),
        out_shape=pltpu.VMEM((count, width), jnp.bfloat16),
        in_specs=[vmem, vmem, hbm, vmem, hbm, hbm],
        out_specs=vmem,
        scratch_shapes=[
            pltpu.VMEM((slots, width), jnp.bfloat16),
            pltpu.VMEM((slots, width), jnp.bfloat16),
            pltpu.VMEM((slots, width), jnp.bfloat16),
            pltpu.VMEM((slots, width), jnp.bfloat16),
            pltpu.VMEM((rows, width), jnp.float32),
            pltpu.VMEM((count, width), jnp.bfloat16),
            pltpu.VMEM((count, slots), jnp.bfloat16),
            pltpu.VMEM((count, 128), jnp.float32),
            pltpu.VMEM((2, width, hidden), jnp.bfloat16),
            pltpu.VMEM((2, hidden, width), jnp.bfloat16),
            sems((3,)),
            sems((2,)),
            sems((2,)),
            sems((n,)),
            sems((n,)),
            sems((n,)),
            sems((n,)),
        ],
        compiler_params=pltpu.CompilerParams(
            collective_id=0, has_side_effects=True, vmem_limit_bytes=60 * 1024 * 1024
        ),
    )(
        expert_ids.reshape(1, count),
        slot_ids.reshape(1, count),
        tokens,
        centroids,
        w_in,
        w_out,
    )


def relay_kernel(
    n,
    cap,
    spare,
    ids_hbm,
    slots_hbm,
    tokens_hbm,
    centroids_hbm,
    w_in_ref,
    w_out_ref,
    out_ref,
    spill_hbm,
    ids_ref,
    slots_ref,
    tokens_ref,
    centroids_ref,
    outgoing,
    pouch,
    inbox,
    expanded,
    received,
    result,
    collected,
    returned,
    place,
    columns,
    full_in,
    full_out,
    flag_out,
    flags_in,
    group_out,
    group_in,
    spill_ref,
    load_sem,
    share_send,
    share_recv,
    send_sem,
    recv_sem,
    back_send,
    back_recv,
    relay_send,
    relay_recv,
    relay_back_send,
    relay_back_recv,
    pouch_send,
    pouch_recv,
    flag_send,
    flag_recv,
    rounds,
    gates,
):
    grp = lax.axis_index("grp")
    me = lax.axis_index("ex")
    half = n // 2
    plane = n // 4
    base = cap // 2
    near_rows = half * cap
    far_rows = half * base
    direct_rows = near_rows + far_rows
    tokens_here, width = tokens_ref.shape
    hidden = full_in.shape[2]
    pieces = hidden // TILE
    partner = {"grp": 1 - grp}

    def peer(slot):
        where = me
        bit = 1
        while bit < n:
            if slot & bit:
                where = where + bit - 2 * bit * ((me // bit) % 2)
            bit *= 2
        return where

    def rows_of(slot):
        if slot < half:
            return slot * cap, cap
        return near_rows + (slot - half) * base, base

    def block(slot):
        return pl.ds(*rows_of(slot))

    def extra(k, start=0):
        return pl.ds(start + k * base, base)

    def remote(src, dst, send, recv, where):
        return pltpu.make_async_remote_copy(
            src_ref=src,
            dst_ref=dst,
            send_sem=send,
            recv_sem=recv,
            device_id=where,
            device_id_type=MESH,
        )

    def dispatch(slot):
        return remote(
            outgoing.at[block(slot), :],
            received.at[block(slot), :],
            send_sem.at[slot],
            recv_sem.at[slot],
            {"ex": peer(slot)},
        )

    def give_back(slot):
        return remote(
            result.at[block(slot), :],
            returned.at[block(slot), :],
            back_send.at[slot],
            back_recv.at[slot],
            {"ex": peer(slot)},
        )

    def forward(k):
        return remote(
            expanded.at[extra(k), :],
            received.at[extra(k, direct_rows), :],
            relay_send.at[k],
            relay_recv.at[k],
            {"ex": peer(k)},
        )

    def give_relay(k):
        return remote(
            result.at[extra(k, direct_rows), :],
            collected.at[extra(k), :],
            relay_back_send.at[k],
            relay_back_recv.at[k],
            {"ex": peer(k)},
        )

    send_pouch = remote(pouch, inbox, pouch_send.at[0], pouch_recv.at[0], {"ex": peer(half)})
    back_pouch = remote(
        expanded.at[pl.ds(0, spare), :],
        returned.at[pl.ds(direct_rows, spare), :],
        pouch_send.at[1],
        pouch_recv.at[1],
        {"ex": peer(half)},
    )

    def send_flag(slot):
        return remote(
            flag_out, flags_in.at[slot], flag_send.at[slot], flag_recv.at[slot], {"ex": peer(slot)}
        )

    swap_flag = remote(group_out, group_in, flag_send.at[0], flag_recv.at[0], partner)

    small = [
        pltpu.make_async_copy(ids_hbm, ids_ref, load_sem.at[0]),
        pltpu.make_async_copy(slots_hbm, slots_ref, load_sem.at[1]),
        pltpu.make_async_copy(tokens_hbm, tokens_ref, load_sem.at[2]),
        pltpu.make_async_copy(centroids_hbm, centroids_ref, load_sem.at[3]),
    ]
    loads = [
        pltpu.make_async_copy(w_in_ref.at[0], full_in.at[0], load_sem.at[4]),
        pltpu.make_async_copy(w_out_ref.at[0], full_out.at[0], load_sem.at[5]),
    ]
    shares = []
    for piece in range(pieces):
        cut = pl.ds(piece * TILE, TILE)
        first = remote(
            w_in_ref.at[0, :, cut],
            full_in.at[1, :, cut],
            share_send.at[0, piece],
            share_recv.at[0, piece],
            partner,
        )
        second = remote(
            w_out_ref.at[0, cut, :],
            full_out.at[1, cut, :],
            share_send.at[1, piece],
            share_recv.at[1, piece],
            partner,
        )
        shares.append((first, second))

    barrier = pltpu.get_barrier_semaphore()
    level = me // plane

    def near_masks(reach):
        return [mask for mask in range(plane) if mask.bit_count() <= reach]

    def call(sem, reach):
        def ring(where):
            pl.semaphore_signal(sem, inc=1, device_id={"ex": where}, device_id_type=MESH)

        for mask in near_masks(reach):
            if mask > 0:
                ring(peer(mask))
        for step in range(1, reach + 1):

            @pl.when(level + step < 4)
            def _():
                for mask in near_masks(reach - step):
                    ring(peer(mask) + step * plane)

            @pl.when(level >= step)
            def _():
                for mask in near_masks(reach - step):
                    ring(peer(mask) - step * plane)

    def answer(sem, reach):
        count = jnp.int32(len(near_masks(reach)) - 1)
        for step in range(1, reach + 1):
            masks = len(near_masks(reach - step))
            count += masks * (level + step < 4).astype(jnp.int32)
            count += masks * (level >= step).astype(jnp.int32)
        pl.semaphore_wait(sem, count)

    def release(gate):
        pl.semaphore_signal(gates.at[gate], inc=1, device_id=partner, device_id_type=MESH)

    for load in small:
        load.start()

    @pl.when(grp == 0)
    def _():
        pl.semaphore_wait(barrier, 1)
        pl.semaphore_signal(gates.at[0], inc=1, device_id=partner, device_id_type=MESH)

    @pl.when(grp == 1)
    def _():
        pl.semaphore_signal(barrier, inc=1, device_id=partner, device_id_type=MESH)
        pl.semaphore_wait(gates.at[0], 1)
        call(barrier, 2)

    for load in loads:
        load.start()
    for pair in shares:
        for share in pair:
            share.start()

    small[0].wait()
    small[1].wait()
    ids = ids_ref[...]
    slots = slots_ref[...]
    offset = jnp.bitwise_xor(ids, me)
    across = offset >= half
    order = (ids * cap + slots).astype(jnp.float32)
    floor = (ids * cap).astype(jnp.float32)
    columns[...] = jnp.broadcast_to(order, (128, tokens_here)).T
    order_column = columns[:, 0:1]
    before = jnp.logical_and(order_column >= floor, order_column < order)
    rank = jnp.sum(jnp.where(before, 1.0, 0.0), axis=0, keepdims=True)
    rank = rank.astype(jnp.int32)
    late = jnp.logical_and(across, rank >= base)
    lines = lax.broadcasted_iota(jnp.int32, (tokens_here, tokens_here), 0)
    lanes = lax.broadcasted_iota(jnp.int32, (tokens_here, tokens_here), 1)
    earlier = (lines < lanes).astype(jnp.bfloat16)
    marks = jnp.broadcast_to(jnp.where(late, 1.0, 0.0), (16, tokens_here)).astype(jnp.bfloat16)
    queue = jnp.dot(marks, earlier, preferred_element_type=jnp.float32)[0:1, :]
    queue = queue.astype(jnp.int32)
    position = jnp.where(
        across,
        jnp.where(late, direct_rows + queue, near_rows + (offset - half) * base + rank),
        offset * cap + slots,
    )
    spill = jnp.max(jnp.where(late, queue + 1, 0), axis=1, keepdims=True) > spare
    flag_out[...] = jnp.broadcast_to(jnp.where(spill, 1.0, 0.0), flag_out.shape)
    flags_in[0] = flag_out[...]

    slot_rows = lax.broadcasted_iota(jnp.int32, (direct_rows + spare, tokens_here), 0)
    hits = slot_rows == position
    spread = hits.astype(jnp.bfloat16)
    target = ((offset - half) * base + rank - base + 1).astype(jnp.float32)
    aim = jnp.sum(jnp.where(hits[direct_rows:], target, 0.0), axis=1, keepdims=True)
    wide = lax.broadcasted_iota(jnp.int32, (spare, 128), 1).astype(jnp.float32)
    pouch[:, width:] = (wide == aim - 1.0).astype(jnp.bfloat16)
    small[2].wait()
    packed = jnp.dot(spread, tokens_ref[...], preferred_element_type=jnp.float32)
    packed = packed.astype(jnp.bfloat16)
    pouch[:, :width] = packed[direct_rows:]
    outgoing[...] = packed[:direct_rows]
    received[block(0), :] = packed[:cap]

    @pl.when(grp == 1)
    def _():
        answer(barrier, 2)
        release(1)
        call(rounds.at[0], 2)

    @pl.when(grp == 0)
    def _():
        pl.semaphore_wait(gates.at[1], 1)

    def settle():
        small[3].wait()
        scores = lax.dot_general(
            centroids_ref[...],
            tokens_ref[...],
            (((1,), (1,)), ((), ())),
            preferred_element_type=jnp.float32,
        )
        experts = lax.broadcasted_iota(jnp.int32, scores.shape, 0)
        chosen = jnp.sum(jnp.where(experts == ids, scores, 0.0), axis=0, keepdims=True)
        gating = 1.0 / (1.0 + jnp.exp(-chosen))
        which = lax.broadcasted_iota(jnp.int32, (128, tokens_here), 0)
        columns[...] = jnp.where(which == 0, position.astype(jnp.float32), gating).T
        slot_columns = lax.broadcasted_iota(jnp.int32, (tokens_here, direct_rows + spare), 1)
        own = columns[:, 0:1].astype(jnp.int32)
        place[...] = (slot_columns == own).astype(jnp.bfloat16)

    def gate(number):
        @pl.when(grp == 1)
        def _():
            answer(rounds.at[number - 2], 2 if number == 2 else 1)
            release(number)
            if number == 2:
                call(rounds.at[1], 1)

        @pl.when(grp == 0)
        def _():
            pl.semaphore_wait(gates.at[number], 1)

    def relay_out():
        send_pouch.wait_recv()
        opened = lax.dot_general(
            inbox[:, width:],
            inbox[:, :width],
            (((0,), (0,)), ((), ())),
            preferred_element_type=jnp.float32,
        )
        opened = opened[:far_rows].astype(jnp.bfloat16)
        expanded[...] = opened
        received[extra(0, direct_rows), :] = opened[:base]
        for k in range(1, half):
            forward(k).start()

    def send_flags():
        for slot in range(1, n):
            send_flag(slot).start()

    def relay_home():
        for k in range(1, half):
            give_relay(k).wait_recv()
            forward(k).wait_send()
        closed = jnp.dot(
            inbox[:, width : width + far_rows],
            collected[...],
            preferred_element_type=jnp.float32,
        )
        expanded[0:spare, :] = closed.astype(jnp.bfloat16)
        back_pouch.start()

    ready = []

    def expert(start, count):
        here = pl.ds(start, count)
        fresh = not ready
        ready.append(True)
        if fresh:
            for load in loads:
                load.wait()
        done = None
        for part in range(2):
            for piece in range(pieces):
                if fresh and part == 1:
                    for share in shares[piece]:
                        share.wait_recv()
                cut = pl.ds(piece * TILE, TILE)
                middle = jnp.dot(
                    received[here, :], full_in[part, :, cut], preferred_element_type=jnp.float32
                )
                middle = jnp.maximum(middle, 0.0).astype(jnp.bfloat16)
                more = jnp.dot(middle, full_out[part, cut, :], preferred_element_type=jnp.float32)
                done = more if done is None else done + more
        done = done.astype(jnp.bfloat16)
        result[here, :] = done
        return done

    def direct_chunk(chosen_slots):
        for slot in chosen_slots:
            if slot > 0:
                dispatch(slot).wait_recv()
        start = rows_of(chosen_slots[0])[0]
        done = expert(start, sum(rows_of(slot)[1] for slot in chosen_slots))
        for slot in chosen_slots:
            if slot > 0:
                give_back(slot).start()
            else:
                returned[block(0), :] = done[:cap]

    def share_flags():
        for slot in range(1, n):
            send_flag(slot).wait_recv()
        group_out[...] = jnp.max(flags_in[...], axis=0)
        for slot in range(1, n):
            send_flag(slot).wait_send()
        swap_flag.start()

    def drain():
        send_pouch.wait_send()
        for slot in range(1, n):
            dispatch(slot).wait_send()
        for pair in shares:
            for share in pair:
                share.wait_send()

    def relayed_chunk():
        for k in range(1, half):
            forward(k).wait_recv()
        done = expert(direct_rows, far_rows)
        collected[extra(0), :] = done[:base]
        for k in range(1, half):
            give_relay(k).start()

    groups = {
        "n0": range(0, plane),
        "n1": range(plane, half),
        "fa": range(half, half + plane),
        "fb": range(half + plane, n),
    }
    steps = {
        "pouch": send_pouch.start,
        "settle": settle,
        "most": lambda: gate(2),
        "all": lambda: gate(3),
        "relay": relay_out,
        "flags": send_flags,
        "relayed": relayed_chunk,
        "home": relay_home,
        "share": share_flags,
        "drain": drain,
    }
    for step in PLAN:
        if step in steps:
            steps[step]()
        elif step in groups:
            direct_chunk(groups[step])
        else:
            dispatch(step).start()

    arrived = jnp.zeros((tokens_here, width), jnp.float32)
    for name in FINISH:
        if name == "spill":
            swap_flag.wait_recv()
            worst = jnp.max(jnp.maximum(group_out[...], group_in[...]))
            spill_ref[0, 0] = worst.astype(jnp.int32)
            tell = pltpu.make_async_copy(spill_ref, spill_hbm, load_sem.at[0])
            tell.start()
            swap_flag.wait_send()
            continue
        if name == "pouch":
            here = pl.ds(direct_rows, spare)
            back_pouch.wait_recv()
        else:
            for slot in groups[name]:
                if slot > 0:
                    give_back(slot).wait_recv()
            here = pl.ds(
                rows_of(groups[name][0])[0], sum(rows_of(slot)[1] for slot in groups[name])
            )
        arrived += jnp.dot(
            place[:, here], returned[here, :], preferred_element_type=jnp.float32
        )
    sums = tokens_ref[...].astype(jnp.float32) + columns[:, 1:2] * arrived
    out_ref[...] = sums.astype(jnp.bfloat16)

    back_pouch.wait_send()
    for k in range(1, half):
        give_relay(k).wait_send()
    for slot in range(1, n):
        give_back(slot).wait_send()
    tell.wait()


def with_relay(n, tokens, expert_ids, slot_ids, centroids, w_in, w_out):
    count, width = tokens.shape
    cap = 2 * count // n
    half = n // 2
    base = cap // 2
    spare = cap + cap // 2
    direct = half * (cap + base)
    hidden = w_in.shape[2]
    hbm = pl.BlockSpec(memory_space=pl.ANY)
    sems = pltpu.SemaphoreType.DMA
    flags = pltpu.SemaphoreType.REGULAR
    bf16 = jnp.bfloat16
    out, spill = pl.pallas_call(
        functools.partial(relay_kernel, n, cap, spare),
        out_shape=[
            pltpu.VMEM((count, width), bf16),
            jax.ShapeDtypeStruct((1, 1), jnp.int32),
        ],
        in_specs=[hbm] * 6,
        out_specs=[pl.BlockSpec(memory_space=pltpu.VMEM), hbm],
        scratch_shapes=[
            pltpu.VMEM((1, count), jnp.int32),
            pltpu.VMEM((1, count), jnp.int32),
            pltpu.VMEM((count, width), bf16),
            pltpu.VMEM(centroids.shape, bf16),
            pltpu.VMEM((direct, width), bf16),
            pltpu.VMEM((spare, width + 128), bf16),
            pltpu.VMEM((spare, width + 128), bf16),
            pltpu.VMEM((half * base, width), bf16),
            pltpu.VMEM((n * cap, width), bf16),
            pltpu.VMEM((n * cap, width), bf16),
            pltpu.VMEM((half * base, width), bf16),
            pltpu.VMEM((direct + spare, width), bf16),
            pltpu.VMEM((count, direct + spare), bf16),
            pltpu.VMEM((count, 128), jnp.float32),
            pltpu.VMEM((2, width, hidden), bf16),
            pltpu.VMEM((2, hidden, width), bf16),
            pltpu.VMEM((8, 128), jnp.float32),
            pltpu.VMEM((n, 8, 128), jnp.float32),
            pltpu.VMEM((8, 128), jnp.float32),
            pltpu.VMEM((8, 128), jnp.float32),
            pltpu.SMEM((1, 1), jnp.int32),
            sems((6,)),
            sems((2, hidden // TILE)),
            sems((2, hidden // TILE)),
            sems((n,)),
            sems((n,)),
            sems((n,)),
            sems((n,)),
            sems((half,)),
            sems((half,)),
            sems((half,)),
            sems((half,)),
            sems((2,)),
            sems((2,)),
            sems((n,)),
            sems((n,)),
            flags((2,)),
            flags((4,)),
        ],
        compiler_params=pltpu.CompilerParams(
            collective_id=1, has_side_effects=True, vmem_limit_bytes=60 * 1024 * 1024
        ),
    )(
        expert_ids.reshape(1, count),
        slot_ids.reshape(1, count),
        tokens,
        centroids,
        w_in,
        w_out,
    )
    return lax.switch(
        spill[0, 0],
        [
            lambda: out,
            lambda: in_one_kernel(n, tokens, expert_ids, slot_ids, centroids, w_in, w_out),
        ],
    )


def in_plain_ops(tokens, expert_ids, slot_ids, centroids, w_in, w_out):
    experts = centroids.shape[0]
    count_rows = tokens.shape[0]
    model_width = tokens.shape[1]
    capacity = 2 * count_rows // experts
    buffer_rows = expert_ids * capacity + slot_ids
    outgoing = (
        jnp.zeros((experts * capacity, model_width), jnp.bfloat16).at[buffer_rows].set(tokens)
    )
    outgoing = outgoing.reshape(experts, capacity, model_width)
    scores = jnp.dot(tokens, centroids.T, preferred_element_type=jnp.float32)
    columns = jnp.arange(experts, dtype=jnp.int32)
    chosen = jnp.sum(jnp.where(columns[None, :] == expert_ids[:, None], scores, 0.0), axis=1)
    gating = jax.nn.sigmoid(chosen)
    full_in, full_out = (
        lax.all_gather(w_in, "grp", axis=2, tiled=True),
        lax.all_gather(w_out, "grp", axis=1, tiled=True),
    )
    received = lax.all_to_all(outgoing, "ex", split_axis=0, concat_axis=0, tiled=True)
    flat_rows = received.reshape(-1, model_width)
    hidden = jnp.maximum(
        jnp.dot(flat_rows, full_in[0], preferred_element_type=jnp.float32), 0.0
    ).astype(jnp.bfloat16)
    result = jnp.dot(hidden, full_out[0], preferred_element_type=jnp.float32)
    returned = lax.all_to_all(
        result.astype(jnp.bfloat16).reshape(received.shape),
        "ex",
        split_axis=0,
        concat_axis=0,
        tiled=True,
    )
    arrived = returned.reshape(-1, model_width)[buffer_rows]
    mixed_rows = tokens.astype(jnp.float32) + gating[:, None] * arrived.astype(jnp.float32)
    return mixed_rows.astype(jnp.bfloat16)


def solution(mesh):
    n = mesh.shape["ex"]

    def on_device(tokens, expert_ids, slot_ids, centroids, w_in, w_out):
        capacity = 2 * tokens.shape[0] // n
        lanes_needed = (n // 2) * (capacity // 2)
        if mesh.shape["grp"] == 2 and n >= 8 and n & (n - 1) == 0 and capacity % 32 == 0 and lanes_needed <= 128:
            return with_relay(n, tokens, expert_ids, slot_ids, centroids, w_in, w_out)
        if mesh.shape["grp"] == 2 and n % 4 == 0 and capacity % 16 == 0:
            return in_one_kernel(n, tokens, expert_ids, slot_ids, centroids, w_in, w_out)
        return in_plain_ops(tokens, expert_ids, slot_ids, centroids, w_in, w_out)

    in_specs = (
        P(("grp", "ex"), None),
        P(("grp", "ex")),
        P(("grp", "ex")),
        P(),
        P("ex", None, "grp"),
        P("ex", "grp", None),
    )
    out_specs = P(("grp", "ex"), None)
    return jax.shard_map(
        on_device, mesh=mesh, in_specs=in_specs, out_specs=out_specs, check_vma=False
    )
```

```python
import functools

import jax
import jax.numpy as jnp
from jax import lax
from jax.experimental import pallas as pl
from jax.experimental.pallas import tpu as pltpu
from jax.sharding import PartitionSpec as P

MESH = pl.DeviceIdType.MESH
TILE = 1024
PLAN = ('pouch', 1, 2, 3, 8, 'settle', 'most', 9, 10, 11, 4, 5, 6, 7, 'relay', 'all', 12, 13, 14, 15, 'flags', 'n0', 'fa', 'n1', 'relayed', 'fb', 'drain', 'home', 'share')
FINISH = ('n0', 'n1', 'fa', 'fb', 'spill', 'pouch')


def expert_kernel(
    n,
    cap,
    ids_ref,
    slots_ref,
    tokens_hbm,
    centroids_ref,
    w_in_ref,
    w_out_ref,
    out_ref,
    outgoing,
    received,
    result,
    returned,
    total,
    tokens_ref,
    place,
    columns,
    full_in,
    full_out,
    load_sem,
    share_send,
    share_recv,
    send_sem,
    recv_sem,
    back_send,
    back_recv,
):
    grp = lax.axis_index("grp")
    me = lax.axis_index("ex")
    half = n // 2
    side = me // half
    seat = me % half
    quarter = n // 4
    rows = quarter * cap
    tokens_here, width = tokens_ref.shape
    hidden = full_in.shape[2]

    def peer_to(slot):
        return ((side + slot // half) % 2) * half + (seat + slot % half) % half

    def peer_from(slot):
        return ((side + slot // half) % 2) * half + (seat + half - slot % half) % half

    def block(slot):
        start = slot * cap
        if not isinstance(slot, int):
            start = pl.multiple_of(start, cap)
        return pl.ds(start, cap)

    barrier = pltpu.get_barrier_semaphore()
    for slot in range(1, n):
        pl.semaphore_signal(
            barrier, inc=1, device_id={"ex": peer_to(slot)}, device_id_type=MESH
        )
    pl.semaphore_signal(barrier, inc=1, device_id={"grp": 1 - grp}, device_id_type=MESH)

    bring = pltpu.make_async_copy(tokens_hbm, tokens_ref, load_sem.at[2])
    bring.start()
    loads = [
        pltpu.make_async_copy(w_in_ref.at[0], full_in.at[0], load_sem.at[0]),
        pltpu.make_async_copy(w_out_ref.at[0], full_out.at[0], load_sem.at[1]),
    ]
    for load in loads:
        load.start()

    ids = ids_ref[...]
    high = (ids >= half).astype(jnp.int32)
    ahead = ids - high * half - seat
    ahead = jnp.where(ahead < 0, ahead + half, ahead)
    across = jnp.where(high == side, 0, 1)
    position = (across * half + ahead) * cap + slots_ref[...]
    slot_rows = lax.broadcasted_iota(jnp.int32, (n * cap, tokens_here), 0)
    spread = (slot_rows == position).astype(jnp.bfloat16)
    bring.wait()
    packed = jnp.dot(spread, tokens_ref[...], preferred_element_type=jnp.float32)
    packed = packed.astype(jnp.bfloat16)
    outgoing[...] = packed
    received[block(0), :] = packed[:cap]

    shares = [
        pltpu.make_async_remote_copy(
            src_ref=w_in_ref.at[0],
            dst_ref=full_in.at[1],
            send_sem=share_send.at[0],
            recv_sem=share_recv.at[0],
            device_id={"grp": 1 - grp},
            device_id_type=MESH,
        ),
        pltpu.make_async_remote_copy(
            src_ref=w_out_ref.at[0],
            dst_ref=full_out.at[1],
            send_sem=share_send.at[1],
            recv_sem=share_recv.at[1],
            device_id={"grp": 1 - grp},
            device_id_type=MESH,
        ),
    ]

    def dispatch(slot):
        return pltpu.make_async_remote_copy(
            src_ref=outgoing.at[block(slot), :],
            dst_ref=received.at[block(slot), :],
            send_sem=send_sem.at[slot],
            recv_sem=recv_sem.at[slot],
            device_id={"ex": peer_to(slot)},
            device_id_type=MESH,
        )

    def give_back(slot):
        return pltpu.make_async_remote_copy(
            src_ref=result.at[block(slot), :],
            dst_ref=returned.at[block(slot), :],
            send_sem=back_send.at[slot],
            recv_sem=back_recv.at[slot],
            device_id={"ex": peer_from(slot)},
            device_id_type=MESH,
        )

    pl.semaphore_wait(barrier, n)
    for step in reversed(range(half)):
        dispatch(half + step).start()
        if step > 0:
            dispatch(step).start()
    for share in shares:
        share.start()

    scores = lax.dot_general(
        centroids_ref[...],
        tokens_ref[...],
        (((1,), (1,)), ((), ())),
        preferred_element_type=jnp.float32,
    )
    experts = lax.broadcasted_iota(jnp.int32, scores.shape, 0)
    chosen = jnp.sum(jnp.where(experts == ids, scores, 0.0), axis=0, keepdims=True)
    gating = 1.0 / (1.0 + jnp.exp(-chosen))
    lines = lax.broadcasted_iota(jnp.int32, (128, tokens_here), 0)
    columns[...] = jnp.where(lines == 0, position.astype(jnp.float32), gating).T
    slot_columns = lax.broadcasted_iota(jnp.int32, (tokens_here, n * cap), 1)
    place[...] = (slot_columns == columns[:, 0:1].astype(jnp.int32)).astype(jnp.bfloat16)

    for load in loads:
        load.wait()
    for share in shares:
        share.wait_recv()

    @pl.loop(0, 4)
    def _(turn):
        chunk = 3 - (2 * turn) % 4 - turn // 2
        first = chunk * quarter

        @pl.loop(0, quarter)
        def _(k):
            @pl.when(first + k > 0)
            def _():
                dispatch(first + k).wait_recv()

        here = pl.ds(pl.multiple_of(chunk * rows, rows), rows)
        total[...] = jnp.zeros_like(total)

        @pl.loop(0, 2 * (hidden // TILE))
        def _(piece):
            part = piece // (hidden // TILE)
            cut = pl.ds(pl.multiple_of((piece % (hidden // TILE)) * TILE, TILE), TILE)
            middle = jnp.dot(
                received[here, :], full_in[part, :, cut], preferred_element_type=jnp.float32
            )
            middle = jnp.maximum(middle, 0.0).astype(jnp.bfloat16)
            total[...] += jnp.dot(
                middle, full_out[part, cut, :], preferred_element_type=jnp.float32
            )

        result[here, :] = total[...].astype(jnp.bfloat16)

        @pl.loop(0, quarter)
        def _(k):
            @pl.when(first + k > 0)
            def _():
                give_back(first + k).start()

            @pl.when(first + k == 0)
            def _():
                returned[block(0), :] = result[block(0), :]

    arrived = jnp.zeros((tokens_here, width), jnp.float32)
    for chunk in (1, 3, 0, 2):
        for slot in range(chunk * quarter, (chunk + 1) * quarter):
            if slot > 0:
                give_back(slot).wait_recv()
        here = pl.ds(chunk * rows, rows)
        arrived += jnp.dot(
            place[:, here], returned[here, :], preferred_element_type=jnp.float32
        )
    mixed = tokens_ref[...].astype(jnp.float32) + columns[:, 1:2] * arrived
    out_ref[...] = mixed.astype(jnp.bfloat16)

    @pl.loop(1, n)
    def _(slot):
        dispatch(slot).wait_send()
        give_back(slot).wait_send()

    for share in shares:
        share.wait_send()


def in_one_kernel(n, tokens, expert_ids, slot_ids, centroids, w_in, w_out):
    count, width = tokens.shape
    cap = 2 * count // n
    slots = n * cap
    rows = slots // 4
    hidden = w_in.shape[2]
    vmem = pl.BlockSpec(memory_space=pltpu.VMEM)
    hbm = pl.BlockSpec(memory_space=pl.ANY)
    sems = pltpu.SemaphoreType.DMA
    return pl.pallas_call(
        functools.partial(expert_kernel, n, cap),
        out_shape=pltpu.VMEM((count, width), jnp.bfloat16),
        in_specs=[vmem, vmem, hbm, vmem, hbm, hbm],
        out_specs=vmem,
        scratch_shapes=[
            pltpu.VMEM((slots, width), jnp.bfloat16),
            pltpu.VMEM((slots, width), jnp.bfloat16),
            pltpu.VMEM((slots, width), jnp.bfloat16),
            pltpu.VMEM((slots, width), jnp.bfloat16),
            pltpu.VMEM((rows, width), jnp.float32),
            pltpu.VMEM((count, width), jnp.bfloat16),
            pltpu.VMEM((count, slots), jnp.bfloat16),
            pltpu.VMEM((count, 128), jnp.float32),
            pltpu.VMEM((2, width, hidden), jnp.bfloat16),
            pltpu.VMEM((2, hidden, width), jnp.bfloat16),
            sems((3,)),
            sems((2,)),
            sems((2,)),
            sems((n,)),
            sems((n,)),
            sems((n,)),
            sems((n,)),
        ],
        compiler_params=pltpu.CompilerParams(
            collective_id=0, has_side_effects=True, vmem_limit_bytes=60 * 1024 * 1024
        ),
    )(
        expert_ids.reshape(1, count),
        slot_ids.reshape(1, count),
        tokens,
        centroids,
        w_in,
        w_out,
    )


def relay_kernel(
    n,
    cap,
    spare,
    ids_hbm,
    slots_hbm,
    tokens_hbm,
    centroids_hbm,
    w_in_ref,
    w_out_ref,
    out_ref,
    spill_hbm,
    ids_ref,
    slots_ref,
    tokens_ref,
    centroids_ref,
    outgoing,
    pouch,
    inbox,
    expanded,
    received,
    result,
    collected,
    returned,
    place,
    columns,
    full_in,
    full_out,
    flag_out,
    flags_in,
    group_out,
    group_in,
    spill_ref,
    load_sem,
    share_send,
    share_recv,
    send_sem,
    recv_sem,
    back_send,
    back_recv,
    relay_send,
    relay_recv,
    relay_back_send,
    relay_back_recv,
    pouch_send,
    pouch_recv,
    flag_send,
    flag_recv,
    rounds,
    gates,
):
    grp = lax.axis_index("grp")
    me = lax.axis_index("ex")
    half = n // 2
    plane = n // 4
    base = cap // 2
    near_rows = half * cap
    far_rows = half * base
    direct_rows = near_rows + far_rows
    tokens_here, width = tokens_ref.shape
    hidden = full_in.shape[2]
    pieces = hidden // TILE
    partner = {"grp": 1 - grp}

    def peer(slot):
        where = me
        bit = 1
        while bit < n:
            if slot & bit:
                where = where + bit - 2 * bit * ((me // bit) % 2)
            bit *= 2
        return where

    def rows_of(slot):
        if slot < half:
            return slot * cap, cap
        return near_rows + (slot - half) * base, base

    def block(slot):
        return pl.ds(*rows_of(slot))

    def extra(k, start=0):
        return pl.ds(start + k * base, base)

    def remote(src, dst, send, recv, where):
        return pltpu.make_async_remote_copy(
            src_ref=src,
            dst_ref=dst,
            send_sem=send,
            recv_sem=recv,
            device_id=where,
            device_id_type=MESH,
        )

    def dispatch(slot):
        return remote(
            outgoing.at[block(slot), :],
            received.at[block(slot), :],
            send_sem.at[0],
            recv_sem.at[slot // plane],
            {"ex": peer(slot)},
        )

    def give_back(slot):
        return remote(
            result.at[block(slot), :],
            returned.at[block(slot), :],
            back_send.at[0],
            back_recv.at[slot // plane],
            {"ex": peer(slot)},
        )

    def forward(k):
        return remote(
            expanded.at[extra(k), :],
            received.at[extra(k, direct_rows), :],
            relay_send.at[0],
            relay_recv.at[0],
            {"ex": peer(k)},
        )

    def give_relay(k):
        return remote(
            result.at[extra(k, direct_rows), :],
            collected.at[extra(k), :],
            relay_back_send.at[0],
            relay_back_recv.at[0],
            {"ex": peer(k)},
        )

    send_pouch = remote(pouch, inbox, pouch_send.at[0], pouch_recv.at[0], {"ex": peer(half)})
    back_pouch = remote(
        expanded.at[pl.ds(0, spare), :],
        returned.at[pl.ds(direct_rows, spare), :],
        pouch_send.at[1],
        pouch_recv.at[1],
        {"ex": peer(half)},
    )

    def send_flag(slot):
        return remote(
            flag_out, flags_in.at[slot], flag_send.at[1], flag_recv.at[1], {"ex": peer(slot)}
        )

    def rows_in_all(first, last):
        start = rows_of(first)[0]
        return pl.ds(start, sum(rows_of(slot)[1] for slot in range(first, last)))

    def many(src, dst, send, recv, first, last):
        here = rows_in_all(first, last)
        return remote(src.at[here, :], dst.at[here, :], send, recv, {"ex": peer(1)})

    def all_sent():
        return many(outgoing, received, send_sem.at[0], recv_sem.at[0], 1, n)

    def all_given():
        return many(result, returned, back_send.at[0], back_recv.at[0], 1, n)

    def landed(group):
        first = max(group * plane, 1)
        return many(
            outgoing, received, send_sem.at[0], recv_sem.at[group], first, (group + 1) * plane
        )

    def came_back(group):
        first = max(group * plane, 1)
        return many(
            result, returned, back_send.at[0], back_recv.at[group], first, (group + 1) * plane
        )

    others = pl.ds(base, far_rows - base)
    all_forward = remote(
        expanded.at[others, :],
        received.at[pl.ds(direct_rows + base, far_rows - base), :],
        relay_send.at[0],
        relay_recv.at[0],
        {"ex": peer(1)},
    )
    all_relay = remote(
        result.at[pl.ds(direct_rows + base, far_rows - base), :],
        collected.at[others, :],
        relay_back_send.at[0],
        relay_back_recv.at[0],
        {"ex": peer(1)},
    )
    all_flags = remote(
        flags_in.at[pl.ds(1, n - 1)],
        flags_in.at[pl.ds(1, n - 1)],
        flag_send.at[1],
        flag_recv.at[1],
        {"ex": peer(1)},
    )

    swap_flag = remote(group_out, group_in, flag_send.at[0], flag_recv.at[0], partner)

    small = [
        pltpu.make_async_copy(ids_hbm, ids_ref, load_sem.at[0]),
        pltpu.make_async_copy(slots_hbm, slots_ref, load_sem.at[1]),
        pltpu.make_async_copy(tokens_hbm, tokens_ref, load_sem.at[2]),
        pltpu.make_async_copy(centroids_hbm, centroids_ref, load_sem.at[3]),
    ]
    loads = [
        pltpu.make_async_copy(w_in_ref.at[0], full_in.at[0], load_sem.at[4]),
        pltpu.make_async_copy(w_out_ref.at[0], full_out.at[0], load_sem.at[5]),
    ]
    shares = []
    for piece in range(pieces):
        cut = pl.ds(piece * TILE, TILE)
        first = remote(
            w_in_ref.at[0, :, cut],
            full_in.at[1, :, cut],
            share_send.at[0],
            share_recv.at[0, piece],
            partner,
        )
        second = remote(
            w_out_ref.at[0, cut, :],
            full_out.at[1, cut, :],
            share_send.at[1],
            share_recv.at[1, piece],
            partner,
        )
        shares.append((first, second))
    sent_in = remote(w_in_ref.at[0], full_in.at[1], share_send.at[0], share_recv.at[0, 0], partner)
    sent_out = remote(
        w_out_ref.at[0], full_out.at[1], share_send.at[1], share_recv.at[1, 0], partner
    )

    barrier = pltpu.get_barrier_semaphore()
    level = me // plane

    def near_masks(reach):
        return [mask for mask in range(plane) if mask.bit_count() <= reach]

    def call(sem, reach):
        def ring(where):
            pl.semaphore_signal(sem, inc=1, device_id={"ex": where}, device_id_type=MESH)

        for mask in near_masks(reach):
            if mask > 0:
                ring(peer(mask))
        for step in range(1, reach + 1):

            @pl.when(level + step < 4)
            def _():
                for mask in near_masks(reach - step):
                    ring(peer(mask) + step * plane)

            @pl.when(level >= step)
            def _():
                for mask in near_masks(reach - step):
                    ring(peer(mask) - step * plane)

    def answer(sem, reach):
        count = jnp.int32(len(near_masks(reach)) - 1)
        for step in range(1, reach + 1):
            masks = len(near_masks(reach - step))
            count += masks * (level + step < 4).astype(jnp.int32)
            count += masks * (level >= step).astype(jnp.int32)
        pl.semaphore_wait(sem, count)

    def release(gate):
        pl.semaphore_signal(gates.at[gate], inc=1, device_id=partner, device_id_type=MESH)

    for load in small:
        load.start()

    @pl.when(grp == 0)
    def _():
        pl.semaphore_wait(barrier, 1)
        pl.semaphore_signal(gates.at[0], inc=1, device_id=partner, device_id_type=MESH)

    @pl.when(grp == 1)
    def _():
        pl.semaphore_signal(barrier, inc=1, device_id=partner, device_id_type=MESH)
        pl.semaphore_wait(gates.at[0], 1)
        call(barrier, 2)

    for load in loads:
        load.start()
    for pair in shares:
        for share in pair:
            share.start()

    small[0].wait()
    small[1].wait()
    ids = ids_ref[...]
    slots = slots_ref[...]
    offset = jnp.bitwise_xor(ids, me)
    across = offset >= half
    order = (ids * cap + slots).astype(jnp.float32)
    floor = (ids * cap).astype(jnp.float32)
    columns[...] = jnp.broadcast_to(order, (128, tokens_here)).T
    order_column = columns[:, 0:1]
    before = jnp.logical_and(order_column >= floor, order_column < order)
    rank = jnp.sum(jnp.where(before, 1.0, 0.0), axis=0, keepdims=True)
    rank = rank.astype(jnp.int32)
    late = jnp.logical_and(across, rank >= base)
    lines = lax.broadcasted_iota(jnp.int32, (tokens_here, tokens_here), 0)
    lanes = lax.broadcasted_iota(jnp.int32, (tokens_here, tokens_here), 1)
    earlier = (lines < lanes).astype(jnp.bfloat16)
    marks = jnp.broadcast_to(jnp.where(late, 1.0, 0.0), (16, tokens_here)).astype(jnp.bfloat16)
    queue = jnp.dot(marks, earlier, preferred_element_type=jnp.float32)[0:1, :]
    queue = queue.astype(jnp.int32)
    position = jnp.where(
        across,
        jnp.where(late, direct_rows + queue, near_rows + (offset - half) * base + rank),
        offset * cap + slots,
    )
    spill = jnp.max(jnp.where(late, queue + 1, 0), axis=1, keepdims=True) > spare
    flag_out[...] = jnp.broadcast_to(jnp.where(spill, 1.0, 0.0), flag_out.shape)
    flags_in[0] = flag_out[...]

    slot_rows = lax.broadcasted_iota(jnp.int32, (direct_rows + spare, tokens_here), 0)
    hits = slot_rows == position
    spread = hits.astype(jnp.bfloat16)
    target = ((offset - half) * base + rank - base + 1).astype(jnp.float32)
    aim = jnp.sum(jnp.where(hits[direct_rows:], target, 0.0), axis=1, keepdims=True)
    wide = lax.broadcasted_iota(jnp.int32, (spare, 128), 1).astype(jnp.float32)
    pouch[:, width:] = (wide == aim - 1.0).astype(jnp.bfloat16)
    small[2].wait()
    packed = jnp.dot(spread, tokens_ref[...], preferred_element_type=jnp.float32)
    packed = packed.astype(jnp.bfloat16)
    pouch[:, :width] = packed[direct_rows:]
    outgoing[...] = packed[:direct_rows]
    received[block(0), :] = packed[:cap]

    @pl.when(grp == 1)
    def _():
        answer(barrier, 2)
        release(1)
        call(rounds.at[0], 2)

    @pl.when(grp == 0)
    def _():
        pl.semaphore_wait(gates.at[1], 1)

    def settle():
        small[3].wait()
        scores = lax.dot_general(
            centroids_ref[...],
            tokens_ref[...],
            (((1,), (1,)), ((), ())),
            preferred_element_type=jnp.float32,
        )
        experts = lax.broadcasted_iota(jnp.int32, scores.shape, 0)
        chosen = jnp.sum(jnp.where(experts == ids, scores, 0.0), axis=0, keepdims=True)
        gating = 1.0 / (1.0 + jnp.exp(-chosen))
        which = lax.broadcasted_iota(jnp.int32, (128, tokens_here), 0)
        columns[...] = jnp.where(which == 0, position.astype(jnp.float32), gating).T
        slot_columns = lax.broadcasted_iota(jnp.int32, (tokens_here, direct_rows + spare), 1)
        own = columns[:, 0:1].astype(jnp.int32)
        place[...] = (slot_columns == own).astype(jnp.bfloat16)

    def gate(number):
        @pl.when(grp == 1)
        def _():
            answer(rounds.at[number - 2], 2 if number == 2 else 1)
            release(number)
            if number == 2:
                call(rounds.at[1], 1)

        @pl.when(grp == 0)
        def _():
            pl.semaphore_wait(gates.at[number], 1)

    def relay_out():
        send_pouch.wait_recv()
        opened = lax.dot_general(
            inbox[:, width:],
            inbox[:, :width],
            (((0,), (0,)), ((), ())),
            preferred_element_type=jnp.float32,
        )
        opened = opened[:far_rows].astype(jnp.bfloat16)
        expanded[...] = opened
        received[extra(0, direct_rows), :] = opened[:base]
        for k in reversed(range(1, half)):
            forward(k).start()

    def send_flags():
        for slot in range(1, n):
            send_flag(slot).start()

    def relay_home():
        all_relay.wait_recv()
        all_forward.wait_send()
        closed = jnp.dot(
            inbox[:, width : width + far_rows],
            collected[...],
            preferred_element_type=jnp.float32,
        )
        expanded[0:spare, :] = closed.astype(jnp.bfloat16)
        back_pouch.start()

    ready = []

    def expert(start, count):
        here = pl.ds(start, count)
        fresh = not ready
        ready.append(True)
        if fresh:
            for load in loads:
                load.wait()
        done = None
        for part in range(2):
            for piece in range(pieces):
                if fresh and part == 1:
                    for share in shares[piece]:
                        share.wait_recv()
                cut = pl.ds(piece * TILE, TILE)
                middle = jnp.dot(
                    received[here, :], full_in[part, :, cut], preferred_element_type=jnp.float32
                )
                middle = jnp.maximum(middle, 0.0).astype(jnp.bfloat16)
                more = jnp.dot(middle, full_out[part, cut, :], preferred_element_type=jnp.float32)
                done = more if done is None else done + more
        done = done.astype(jnp.bfloat16)
        result[here, :] = done
        return done

    def direct_chunk(chosen_slots):
        for group in sorted({slot // plane for slot in chosen_slots}):
            landed(group).wait_recv()
        start = rows_of(chosen_slots[0])[0]
        done = expert(start, sum(rows_of(slot)[1] for slot in chosen_slots))
        for slot in chosen_slots:
            if slot > 0:
                give_back(slot).start()
            else:
                returned[block(0), :] = done[:cap]

    def share_flags():
        all_flags.wait_recv()
        group_out[...] = jnp.max(flags_in[...], axis=0)
        all_flags.wait_send()
        swap_flag.start()

    def drain():
        send_pouch.wait_send()
        all_sent().wait_send()
        sent_in.wait_send()
        sent_out.wait_send()

    def relayed_chunk():
        all_forward.wait_recv()
        done = expert(direct_rows, far_rows)
        collected[extra(0), :] = done[:base]
        for k in reversed(range(1, half)):
            give_relay(k).start()

    groups = {
        "n0": range(0, plane),
        "n1": range(plane, half),
        "fa": range(half, half + plane),
        "fb": range(half + plane, n),
        "ff": range(half, n),
    }
    steps = {
        "pouch": send_pouch.start,
        "settle": settle,
        "most": lambda: gate(2),
        "all": lambda: gate(3),
        "relay": relay_out,
        "flags": send_flags,
        "relayed": relayed_chunk,
        "home": relay_home,
        "share": share_flags,
        "drain": drain,
    }
    for step in PLAN:
        if step in steps:
            steps[step]()
        elif step in groups:
            direct_chunk(groups[step])
        else:
            dispatch(step).start()

    arrived = jnp.zeros((tokens_here, width), jnp.float32)
    for name in FINISH:
        if name == "spill":
            swap_flag.wait_recv()
            worst = jnp.max(jnp.maximum(group_out[...], group_in[...]))
            spill_ref[0, 0] = worst.astype(jnp.int32)
            tell = pltpu.make_async_copy(spill_ref, spill_hbm, load_sem.at[0])
            tell.start()
            swap_flag.wait_send()
            continue
        if name == "pouch":
            here = pl.ds(direct_rows, spare)
            back_pouch.wait_recv()
        else:
            for group in sorted({slot // plane for slot in groups[name]}):
                came_back(group).wait_recv()
            here = rows_in_all(groups[name][0], groups[name][-1] + 1)
        arrived += jnp.dot(
            place[:, here], returned[here, :], preferred_element_type=jnp.float32
        )
    sums = tokens_ref[...].astype(jnp.float32) + columns[:, 1:2] * arrived
    out_ref[...] = sums.astype(jnp.bfloat16)

    back_pouch.wait_send()
    all_relay.wait_send()
    all_given().wait_send()
    tell.wait()


def with_relay(n, tokens, expert_ids, slot_ids, centroids, w_in, w_out):
    count, width = tokens.shape
    cap = 2 * count // n
    half = n // 2
    base = cap // 2
    spare = cap + cap // 2
    direct = half * (cap + base)
    hidden = w_in.shape[2]
    hbm = pl.BlockSpec(memory_space=pl.ANY)
    sems = pltpu.SemaphoreType.DMA
    flags = pltpu.SemaphoreType.REGULAR
    bf16 = jnp.bfloat16
    out, spill = pl.pallas_call(
        functools.partial(relay_kernel, n, cap, spare),
        out_shape=[
            pltpu.VMEM((count, width), bf16),
            jax.ShapeDtypeStruct((1, 1), jnp.int32),
        ],
        in_specs=[hbm] * 6,
        out_specs=[pl.BlockSpec(memory_space=pltpu.VMEM), hbm],
        scratch_shapes=[
            pltpu.VMEM((1, count), jnp.int32),
            pltpu.VMEM((1, count), jnp.int32),
            pltpu.VMEM((count, width), bf16),
            pltpu.VMEM(centroids.shape, bf16),
            pltpu.VMEM((direct, width), bf16),
            pltpu.VMEM((spare, width + 128), bf16),
            pltpu.VMEM((spare, width + 128), bf16),
            pltpu.VMEM((half * base, width), bf16),
            pltpu.VMEM((n * cap, width), bf16),
            pltpu.VMEM((n * cap, width), bf16),
            pltpu.VMEM((half * base, width), bf16),
            pltpu.VMEM((direct + spare, width), bf16),
            pltpu.VMEM((count, direct + spare), bf16),
            pltpu.VMEM((count, 128), jnp.float32),
            pltpu.VMEM((2, width, hidden), bf16),
            pltpu.VMEM((2, hidden, width), bf16),
            pltpu.VMEM((8, 128), jnp.float32),
            pltpu.VMEM((n, 8, 128), jnp.float32),
            pltpu.VMEM((8, 128), jnp.float32),
            pltpu.VMEM((8, 128), jnp.float32),
            pltpu.SMEM((1, 1), jnp.int32),
            sems((6,)),
            sems((2,)),
            sems((2, hidden // TILE)),
            sems((1,)),
            sems((4,)),
            sems((1,)),
            sems((4,)),
            sems((1,)),
            sems((1,)),
            sems((1,)),
            sems((1,)),
            sems((2,)),
            sems((2,)),
            sems((2,)),
            sems((2,)),
            flags((2,)),
            flags((4,)),
        ],
        compiler_params=pltpu.CompilerParams(
            collective_id=1, has_side_effects=True, vmem_limit_bytes=60 * 1024 * 1024
        ),
    )(
        expert_ids.reshape(1, count),
        slot_ids.reshape(1, count),
        tokens,
        centroids,
        w_in,
        w_out,
    )
    return lax.switch(
        spill[0, 0],
        [
            lambda: out,
            lambda: in_one_kernel(n, tokens, expert_ids, slot_ids, centroids, w_in, w_out),
        ],
    )


def in_plain_ops(tokens, expert_ids, slot_ids, centroids, w_in, w_out):
    experts = centroids.shape[0]
    count_rows = tokens.shape[0]
    model_width = tokens.shape[1]
    capacity = 2 * count_rows // experts
    buffer_rows = expert_ids * capacity + slot_ids
    outgoing = (
        jnp.zeros((experts * capacity, model_width), jnp.bfloat16).at[buffer_rows].set(tokens)
    )
    outgoing = outgoing.reshape(experts, capacity, model_width)
    scores = jnp.dot(tokens, centroids.T, preferred_element_type=jnp.float32)
    columns = jnp.arange(experts, dtype=jnp.int32)
    chosen = jnp.sum(jnp.where(columns[None, :] == expert_ids[:, None], scores, 0.0), axis=1)
    gating = jax.nn.sigmoid(chosen)
    full_in, full_out = (
        lax.all_gather(w_in, "grp", axis=2, tiled=True),
        lax.all_gather(w_out, "grp", axis=1, tiled=True),
    )
    received = lax.all_to_all(outgoing, "ex", split_axis=0, concat_axis=0, tiled=True)
    flat_rows = received.reshape(-1, model_width)
    hidden = jnp.maximum(
        jnp.dot(flat_rows, full_in[0], preferred_element_type=jnp.float32), 0.0
    ).astype(jnp.bfloat16)
    result = jnp.dot(hidden, full_out[0], preferred_element_type=jnp.float32)
    returned = lax.all_to_all(
        result.astype(jnp.bfloat16).reshape(received.shape),
        "ex",
        split_axis=0,
        concat_axis=0,
        tiled=True,
    )
    arrived = returned.reshape(-1, model_width)[buffer_rows]
    mixed_rows = tokens.astype(jnp.float32) + gating[:, None] * arrived.astype(jnp.float32)
    return mixed_rows.astype(jnp.bfloat16)


def solution(mesh):
    n = mesh.shape["ex"]

    def on_device(tokens, expert_ids, slot_ids, centroids, w_in, w_out):
        capacity = 2 * tokens.shape[0] // n
        lanes_needed = (n // 2) * (capacity // 2)
        if mesh.shape["grp"] == 2 and n >= 8 and n & (n - 1) == 0 and capacity % 32 == 0 and lanes_needed <= 128:
            return with_relay(n, tokens, expert_ids, slot_ids, centroids, w_in, w_out)
        if mesh.shape["grp"] == 2 and n % 4 == 0 and capacity % 16 == 0:
            return in_one_kernel(n, tokens, expert_ids, slot_ids, centroids, w_in, w_out)
        return in_plain_ops(tokens, expert_ids, slot_ids, centroids, w_in, w_out)

    in_specs = (
        P(("grp", "ex"), None),
        P(("grp", "ex")),
        P(("grp", "ex")),
        P(),
        P("ex", None, "grp"),
        P("ex", "grp", None),
    )
    out_specs = P(("grp", "ex"), None)
    return jax.shard_map(
        on_device, mesh=mesh, in_specs=in_specs, out_specs=out_specs, check_vma=False
    )
```

```python
import functools

import jax
import jax.numpy as jnp
from jax import lax
from jax.experimental import pallas as pl
from jax.experimental.pallas import tpu as pltpu
from jax.extend.core.primitives import cond_p
from jax.sharding import PartitionSpec as P

MESH = pl.DeviceIdType.MESH
TILE = 1024
PLAN = ('pouch', 1, 2, 3, 8, 'settle', 'most', 9, 10, 11, 4, 5, 6, 7, 'relay', 'all', 12, 13, 14, 15, 'flags', 'n0', 'fa', 'n1', 'relayed', 'fb', 'drain', 'home', 'share')
FINISH = ('n0', 'n1', 'fa', 'fb', 'spill', 'pouch')


def expert_kernel(
    n,
    cap,
    ids_ref,
    slots_ref,
    tokens_hbm,
    centroids_ref,
    w_in_ref,
    w_out_ref,
    out_ref,
    outgoing,
    received,
    result,
    returned,
    total,
    tokens_ref,
    place,
    columns,
    full_in,
    full_out,
    load_sem,
    share_send,
    share_recv,
    send_sem,
    recv_sem,
    back_send,
    back_recv,
):
    grp = lax.axis_index("grp")
    me = lax.axis_index("ex")
    half = n // 2
    side = me // half
    seat = me % half
    quarter = n // 4
    rows = quarter * cap
    tokens_here, width = tokens_ref.shape
    hidden = full_in.shape[2]

    def peer_to(slot):
        return ((side + slot // half) % 2) * half + (seat + slot % half) % half

    def peer_from(slot):
        return ((side + slot // half) % 2) * half + (seat + half - slot % half) % half

    def block(slot):
        start = slot * cap
        if not isinstance(slot, int):
            start = pl.multiple_of(start, cap)
        return pl.ds(start, cap)

    barrier = pltpu.get_barrier_semaphore()
    for slot in range(1, n):
        pl.semaphore_signal(
            barrier, inc=1, device_id={"ex": peer_to(slot)}, device_id_type=MESH
        )
    pl.semaphore_signal(barrier, inc=1, device_id={"grp": 1 - grp}, device_id_type=MESH)

    bring = pltpu.make_async_copy(tokens_hbm, tokens_ref, load_sem.at[2])
    bring.start()
    loads = [
        pltpu.make_async_copy(w_in_ref.at[0], full_in.at[0], load_sem.at[0]),
        pltpu.make_async_copy(w_out_ref.at[0], full_out.at[0], load_sem.at[1]),
    ]
    for load in loads:
        load.start()

    ids = ids_ref[...]
    high = (ids >= half).astype(jnp.int32)
    ahead = ids - high * half - seat
    ahead = jnp.where(ahead < 0, ahead + half, ahead)
    across = jnp.where(high == side, 0, 1)
    position = (across * half + ahead) * cap + slots_ref[...]
    slot_rows = lax.broadcasted_iota(jnp.int32, (n * cap, tokens_here), 0)
    spread = (slot_rows == position).astype(jnp.bfloat16)
    bring.wait()
    packed = jnp.dot(spread, tokens_ref[...], preferred_element_type=jnp.float32)
    packed = packed.astype(jnp.bfloat16)
    outgoing[...] = packed
    received[block(0), :] = packed[:cap]

    shares = [
        pltpu.make_async_remote_copy(
            src_ref=w_in_ref.at[0],
            dst_ref=full_in.at[1],
            send_sem=share_send.at[0],
            recv_sem=share_recv.at[0],
            device_id={"grp": 1 - grp},
            device_id_type=MESH,
        ),
        pltpu.make_async_remote_copy(
            src_ref=w_out_ref.at[0],
            dst_ref=full_out.at[1],
            send_sem=share_send.at[1],
            recv_sem=share_recv.at[1],
            device_id={"grp": 1 - grp},
            device_id_type=MESH,
        ),
    ]

    def dispatch(slot):
        return pltpu.make_async_remote_copy(
            src_ref=outgoing.at[block(slot), :],
            dst_ref=received.at[block(slot), :],
            send_sem=send_sem.at[slot],
            recv_sem=recv_sem.at[slot],
            device_id={"ex": peer_to(slot)},
            device_id_type=MESH,
        )

    def give_back(slot):
        return pltpu.make_async_remote_copy(
            src_ref=result.at[block(slot), :],
            dst_ref=returned.at[block(slot), :],
            send_sem=back_send.at[slot],
            recv_sem=back_recv.at[slot],
            device_id={"ex": peer_from(slot)},
            device_id_type=MESH,
        )

    pl.semaphore_wait(barrier, n)
    for step in reversed(range(half)):
        dispatch(half + step).start()
        if step > 0:
            dispatch(step).start()
    for share in shares:
        share.start()

    scores = lax.dot_general(
        centroids_ref[...],
        tokens_ref[...],
        (((1,), (1,)), ((), ())),
        preferred_element_type=jnp.float32,
    )
    experts = lax.broadcasted_iota(jnp.int32, scores.shape, 0)
    chosen = jnp.sum(jnp.where(experts == ids, scores, 0.0), axis=0, keepdims=True)
    gating = 1.0 / (1.0 + jnp.exp(-chosen))
    lines = lax.broadcasted_iota(jnp.int32, (128, tokens_here), 0)
    columns[...] = jnp.where(lines == 0, position.astype(jnp.float32), gating).T
    slot_columns = lax.broadcasted_iota(jnp.int32, (tokens_here, n * cap), 1)
    place[...] = (slot_columns == columns[:, 0:1].astype(jnp.int32)).astype(jnp.bfloat16)

    for load in loads:
        load.wait()
    for share in shares:
        share.wait_recv()

    @pl.loop(0, 4)
    def _(turn):
        chunk = 3 - (2 * turn) % 4 - turn // 2
        first = chunk * quarter

        @pl.loop(0, quarter)
        def _(k):
            @pl.when(first + k > 0)
            def _():
                dispatch(first + k).wait_recv()

        here = pl.ds(pl.multiple_of(chunk * rows, rows), rows)
        total[...] = jnp.zeros_like(total)

        @pl.loop(0, 2 * (hidden // TILE))
        def _(piece):
            part = piece // (hidden // TILE)
            cut = pl.ds(pl.multiple_of((piece % (hidden // TILE)) * TILE, TILE), TILE)
            middle = jnp.dot(
                received[here, :], full_in[part, :, cut], preferred_element_type=jnp.float32
            )
            middle = jnp.maximum(middle, 0.0).astype(jnp.bfloat16)
            total[...] += jnp.dot(
                middle, full_out[part, cut, :], preferred_element_type=jnp.float32
            )

        result[here, :] = total[...].astype(jnp.bfloat16)

        @pl.loop(0, quarter)
        def _(k):
            @pl.when(first + k > 0)
            def _():
                give_back(first + k).start()

            @pl.when(first + k == 0)
            def _():
                returned[block(0), :] = result[block(0), :]

    arrived = jnp.zeros((tokens_here, width), jnp.float32)
    for chunk in (1, 3, 0, 2):
        for slot in range(chunk * quarter, (chunk + 1) * quarter):
            if slot > 0:
                give_back(slot).wait_recv()
        here = pl.ds(chunk * rows, rows)
        arrived += jnp.dot(
            place[:, here], returned[here, :], preferred_element_type=jnp.float32
        )
    mixed = tokens_ref[...].astype(jnp.float32) + columns[:, 1:2] * arrived
    out_ref[...] = mixed.astype(jnp.bfloat16)

    @pl.loop(1, n)
    def _(slot):
        dispatch(slot).wait_send()
        give_back(slot).wait_send()

    for share in shares:
        share.wait_send()


def in_one_kernel(n, tokens, expert_ids, slot_ids, centroids, w_in, w_out):
    count, width = tokens.shape
    cap = 2 * count // n
    slots = n * cap
    rows = slots // 4
    hidden = w_in.shape[2]
    vmem = pl.BlockSpec(memory_space=pltpu.VMEM)
    hbm = pl.BlockSpec(memory_space=pl.ANY)
    sems = pltpu.SemaphoreType.DMA
    return pl.pallas_call(
        functools.partial(expert_kernel, n, cap),
        out_shape=pltpu.VMEM((count, width), jnp.bfloat16),
        in_specs=[vmem, vmem, hbm, vmem, hbm, hbm],
        out_specs=vmem,
        scratch_shapes=[
            pltpu.VMEM((slots, width), jnp.bfloat16),
            pltpu.VMEM((slots, width), jnp.bfloat16),
            pltpu.VMEM((slots, width), jnp.bfloat16),
            pltpu.VMEM((slots, width), jnp.bfloat16),
            pltpu.VMEM((rows, width), jnp.float32),
            pltpu.VMEM((count, width), jnp.bfloat16),
            pltpu.VMEM((count, slots), jnp.bfloat16),
            pltpu.VMEM((count, 128), jnp.float32),
            pltpu.VMEM((2, width, hidden), jnp.bfloat16),
            pltpu.VMEM((2, hidden, width), jnp.bfloat16),
            sems((3,)),
            sems((2,)),
            sems((2,)),
            sems((n,)),
            sems((n,)),
            sems((n,)),
            sems((n,)),
        ],
        compiler_params=pltpu.CompilerParams(
            collective_id=0, has_side_effects=True, vmem_limit_bytes=60 * 1024 * 1024
        ),
    )(
        expert_ids.reshape(1, count),
        slot_ids.reshape(1, count),
        tokens,
        centroids,
        w_in,
        w_out,
    )


def relay_kernel(
    n,
    cap,
    spare,
    ids_hbm,
    slots_hbm,
    tokens_hbm,
    centroids_hbm,
    w_in_ref,
    w_out_ref,
    out_ref,
    spill_hbm,
    ids_ref,
    slots_ref,
    tokens_ref,
    centroids_ref,
    outgoing,
    pouch,
    inbox,
    expanded,
    received,
    result,
    collected,
    returned,
    place,
    columns,
    full_in,
    full_out,
    flag_out,
    flags_in,
    group_out,
    group_in,
    spill_ref,
    load_sem,
    share_send,
    share_recv,
    send_sem,
    recv_sem,
    back_send,
    back_recv,
    relay_send,
    relay_recv,
    relay_back_send,
    relay_back_recv,
    pouch_send,
    pouch_recv,
    flag_send,
    flag_recv,
    rounds,
    gates,
):
    grp = lax.axis_index("grp")
    me = lax.axis_index("ex")
    half = n // 2
    plane = n // 4
    base = cap // 2
    near_rows = half * cap
    far_rows = half * base
    direct_rows = near_rows + far_rows
    tokens_here, width = tokens_ref.shape
    hidden = full_in.shape[2]
    pieces = hidden // TILE
    partner = {"grp": 1 - grp}

    def peer(slot):
        where = me
        bit = 1
        while bit < n:
            if slot & bit:
                where = where + bit - 2 * bit * ((me // bit) % 2)
            bit *= 2
        return where

    def rows_of(slot):
        if slot < half:
            return slot * cap, cap
        return near_rows + (slot - half) * base, base

    def block(slot):
        return pl.ds(*rows_of(slot))

    def extra(k, start=0):
        return pl.ds(start + k * base, base)

    def remote(src, dst, send, recv, where):
        return pltpu.make_async_remote_copy(
            src_ref=src,
            dst_ref=dst,
            send_sem=send,
            recv_sem=recv,
            device_id=where,
            device_id_type=MESH,
        )

    def dispatch(slot):
        return remote(
            outgoing.at[block(slot), :],
            received.at[block(slot), :],
            send_sem.at[0],
            recv_sem.at[slot // plane],
            {"ex": peer(slot)},
        )

    def give_back(slot):
        return remote(
            result.at[block(slot), :],
            returned.at[block(slot), :],
            back_send.at[0],
            back_recv.at[slot // plane],
            {"ex": peer(slot)},
        )

    def forward(k):
        return remote(
            expanded.at[extra(k), :],
            received.at[extra(k, direct_rows), :],
            relay_send.at[0],
            relay_recv.at[0],
            {"ex": peer(k)},
        )

    def give_relay(k):
        return remote(
            result.at[extra(k, direct_rows), :],
            collected.at[extra(k), :],
            relay_back_send.at[0],
            relay_back_recv.at[0],
            {"ex": peer(k)},
        )

    send_pouch = remote(pouch, inbox, pouch_send.at[0], pouch_recv.at[0], {"ex": peer(half)})
    back_pouch = remote(
        expanded.at[pl.ds(0, spare), :],
        returned.at[pl.ds(direct_rows, spare), :],
        pouch_send.at[1],
        pouch_recv.at[1],
        {"ex": peer(half)},
    )

    def send_flag(slot):
        return remote(
            flag_out, flags_in.at[slot], flag_send.at[1], flag_recv.at[1], {"ex": peer(slot)}
        )

    def rows_in_all(first, last):
        start = rows_of(first)[0]
        return pl.ds(start, sum(rows_of(slot)[1] for slot in range(first, last)))

    def many(src, dst, send, recv, first, last):
        here = rows_in_all(first, last)
        return remote(src.at[here, :], dst.at[here, :], send, recv, {"ex": peer(1)})

    def all_sent():
        return many(outgoing, received, send_sem.at[0], recv_sem.at[0], 1, n)

    def all_given():
        return many(result, returned, back_send.at[0], back_recv.at[0], 1, n)

    def landed(group):
        first = max(group * plane, 1)
        return many(
            outgoing, received, send_sem.at[0], recv_sem.at[group], first, (group + 1) * plane
        )

    def came_back(group):
        first = max(group * plane, 1)
        return many(
            result, returned, back_send.at[0], back_recv.at[group], first, (group + 1) * plane
        )

    others = pl.ds(base, far_rows - base)
    all_forward = remote(
        expanded.at[others, :],
        received.at[pl.ds(direct_rows + base, far_rows - base), :],
        relay_send.at[0],
        relay_recv.at[0],
        {"ex": peer(1)},
    )
    all_relay = remote(
        result.at[pl.ds(direct_rows + base, far_rows - base), :],
        collected.at[others, :],
        relay_back_send.at[0],
        relay_back_recv.at[0],
        {"ex": peer(1)},
    )
    all_flags = remote(
        flags_in.at[pl.ds(1, n - 1)],
        flags_in.at[pl.ds(1, n - 1)],
        flag_send.at[1],
        flag_recv.at[1],
        {"ex": peer(1)},
    )

    swap_flag = remote(group_out, group_in, flag_send.at[0], flag_recv.at[0], partner)

    small = [
        pltpu.make_async_copy(ids_hbm, ids_ref, load_sem.at[0]),
        pltpu.make_async_copy(slots_hbm, slots_ref, load_sem.at[1]),
        pltpu.make_async_copy(tokens_hbm, tokens_ref, load_sem.at[2]),
        pltpu.make_async_copy(centroids_hbm, centroids_ref, load_sem.at[3]),
    ]
    loads = [
        pltpu.make_async_copy(w_in_ref.at[0], full_in.at[0], load_sem.at[4]),
        pltpu.make_async_copy(w_out_ref.at[0], full_out.at[0], load_sem.at[5]),
    ]
    shares = []
    for piece in range(pieces):
        cut = pl.ds(piece * TILE, TILE)
        first = remote(
            w_in_ref.at[0, :, cut],
            full_in.at[1, :, cut],
            share_send.at[0],
            share_recv.at[0, piece],
            partner,
        )
        second = remote(
            w_out_ref.at[0, cut, :],
            full_out.at[1, cut, :],
            share_send.at[1],
            share_recv.at[1, piece],
            partner,
        )
        shares.append((first, second))
    sent_in = remote(w_in_ref.at[0], full_in.at[1], share_send.at[0], share_recv.at[0, 0], partner)
    sent_out = remote(
        w_out_ref.at[0], full_out.at[1], share_send.at[1], share_recv.at[1, 0], partner
    )

    barrier = pltpu.get_barrier_semaphore()
    level = me // plane

    def near_masks(reach):
        return [mask for mask in range(plane) if mask.bit_count() <= reach]

    def call(sem, reach):
        def ring(where):
            pl.semaphore_signal(sem, inc=1, device_id={"ex": where}, device_id_type=MESH)

        for mask in near_masks(reach):
            if mask > 0:
                ring(peer(mask))
        for step in range(1, reach + 1):

            @pl.when(level + step < 4)
            def _():
                for mask in near_masks(reach - step):
                    ring(peer(mask) + step * plane)

            @pl.when(level >= step)
            def _():
                for mask in near_masks(reach - step):
                    ring(peer(mask) - step * plane)

    def answer(sem, reach):
        count = jnp.int32(len(near_masks(reach)) - 1)
        for step in range(1, reach + 1):
            masks = len(near_masks(reach - step))
            count += masks * (level + step < 4).astype(jnp.int32)
            count += masks * (level >= step).astype(jnp.int32)
        pl.semaphore_wait(sem, count)

    def release(gate):
        pl.semaphore_signal(gates.at[gate], inc=1, device_id=partner, device_id_type=MESH)

    for load in small:
        load.start()

    @pl.when(grp == 0)
    def _():
        pl.semaphore_wait(barrier, 1)
        pl.semaphore_signal(gates.at[0], inc=1, device_id=partner, device_id_type=MESH)

    @pl.when(grp == 1)
    def _():
        pl.semaphore_signal(barrier, inc=1, device_id=partner, device_id_type=MESH)
        pl.semaphore_wait(gates.at[0], 1)
        call(barrier, 2)

    for load in loads:
        load.start()
    for pair in shares:
        for share in pair:
            share.start()

    small[0].wait()
    small[1].wait()
    ids = ids_ref[...]
    slots = slots_ref[...]
    offset = jnp.bitwise_xor(ids, me)
    across = offset >= half
    order = (ids * cap + slots).astype(jnp.float32)
    floor = (ids * cap).astype(jnp.float32)
    columns[...] = jnp.broadcast_to(order, (128, tokens_here)).T
    order_column = columns[:, 0:1]
    before = jnp.logical_and(order_column >= floor, order_column < order)
    rank = jnp.sum(jnp.where(before, 1.0, 0.0), axis=0, keepdims=True)
    rank = rank.astype(jnp.int32)
    late = jnp.logical_and(across, rank >= base)
    lines = lax.broadcasted_iota(jnp.int32, (tokens_here, tokens_here), 0)
    lanes = lax.broadcasted_iota(jnp.int32, (tokens_here, tokens_here), 1)
    earlier = (lines < lanes).astype(jnp.bfloat16)
    marks = jnp.broadcast_to(jnp.where(late, 1.0, 0.0), (16, tokens_here)).astype(jnp.bfloat16)
    queue = jnp.dot(marks, earlier, preferred_element_type=jnp.float32)[0:1, :]
    queue = queue.astype(jnp.int32)
    position = jnp.where(
        across,
        jnp.where(late, direct_rows + queue, near_rows + (offset - half) * base + rank),
        offset * cap + slots,
    )
    spill = jnp.max(jnp.where(late, queue + 1, 0), axis=1, keepdims=True) > spare
    flag_out[...] = jnp.broadcast_to(jnp.where(spill, 1.0, 0.0), flag_out.shape)
    flags_in[0] = flag_out[...]

    slot_rows = lax.broadcasted_iota(jnp.int32, (direct_rows + spare, tokens_here), 0)
    hits = slot_rows == position
    spread = hits.astype(jnp.bfloat16)
    target = ((offset - half) * base + rank - base + 1).astype(jnp.float32)
    aim = jnp.sum(jnp.where(hits[direct_rows:], target, 0.0), axis=1, keepdims=True)
    wide = lax.broadcasted_iota(jnp.int32, (spare, 128), 1).astype(jnp.float32)
    pouch[:, width:] = (wide == aim - 1.0).astype(jnp.bfloat16)
    small[2].wait()
    packed = jnp.dot(spread, tokens_ref[...], preferred_element_type=jnp.float32)
    packed = packed.astype(jnp.bfloat16)
    pouch[:, :width] = packed[direct_rows:]
    outgoing[...] = packed[:direct_rows]
    received[block(0), :] = packed[:cap]

    @pl.when(grp == 1)
    def _():
        answer(barrier, 2)
        release(1)
        call(rounds.at[0], 2)

    @pl.when(grp == 0)
    def _():
        pl.semaphore_wait(gates.at[1], 1)

    def settle():
        small[3].wait()
        scores = lax.dot_general(
            centroids_ref[...],
            tokens_ref[...],
            (((1,), (1,)), ((), ())),
            preferred_element_type=jnp.float32,
        )
        experts = lax.broadcasted_iota(jnp.int32, scores.shape, 0)
        chosen = jnp.sum(jnp.where(experts == ids, scores, 0.0), axis=0, keepdims=True)
        gating = 1.0 / (1.0 + jnp.exp(-chosen))
        which = lax.broadcasted_iota(jnp.int32, (128, tokens_here), 0)
        columns[...] = jnp.where(which == 0, position.astype(jnp.float32), gating).T
        slot_columns = lax.broadcasted_iota(jnp.int32, (tokens_here, direct_rows + spare), 1)
        own = columns[:, 0:1].astype(jnp.int32)
        place[...] = (slot_columns == own).astype(jnp.bfloat16)

    def gate(number):
        @pl.when(grp == 1)
        def _():
            answer(rounds.at[number - 2], 2 if number == 2 else 1)
            release(number)
            if number == 2:
                call(rounds.at[1], 1)

        @pl.when(grp == 0)
        def _():
            pl.semaphore_wait(gates.at[number], 1)

    def relay_out():
        send_pouch.wait_recv()
        opened = lax.dot_general(
            inbox[:, width:],
            inbox[:, :width],
            (((0,), (0,)), ((), ())),
            preferred_element_type=jnp.float32,
        )
        opened = opened[:far_rows].astype(jnp.bfloat16)
        expanded[...] = opened
        received[extra(0, direct_rows), :] = opened[:base]
        for k in reversed(range(1, half)):
            forward(k).start()

    def send_flags():
        for slot in range(1, n):
            send_flag(slot).start()

    def relay_home():
        all_relay.wait_recv()
        all_forward.wait_send()
        closed = jnp.dot(
            inbox[:, width : width + far_rows],
            collected[...],
            preferred_element_type=jnp.float32,
        )
        expanded[0:spare, :] = closed.astype(jnp.bfloat16)
        back_pouch.start()

    ready = []

    def expert(start, count):
        here = pl.ds(start, count)
        fresh = not ready
        ready.append(True)
        if fresh:
            for load in loads:
                load.wait()
        done = None
        for part in range(2):
            for piece in range(pieces):
                if fresh and part == 1:
                    for share in shares[piece]:
                        share.wait_recv()
                cut = pl.ds(piece * TILE, TILE)
                middle = jnp.dot(
                    received[here, :], full_in[part, :, cut], preferred_element_type=jnp.float32
                )
                middle = jnp.maximum(middle, 0.0).astype(jnp.bfloat16)
                more = jnp.dot(middle, full_out[part, cut, :], preferred_element_type=jnp.float32)
                done = more if done is None else done + more
        done = done.astype(jnp.bfloat16)
        result[here, :] = done
        return done

    def direct_chunk(chosen_slots):
        for group in sorted({slot // plane for slot in chosen_slots}):
            landed(group).wait_recv()
        start = rows_of(chosen_slots[0])[0]
        done = expert(start, sum(rows_of(slot)[1] for slot in chosen_slots))
        for slot in chosen_slots:
            if slot > 0:
                give_back(slot).start()
            else:
                returned[block(0), :] = done[:cap]

    def share_flags():
        all_flags.wait_recv()
        group_out[...] = jnp.max(flags_in[...], axis=0)
        all_flags.wait_send()
        swap_flag.start()

    def drain():
        send_pouch.wait_send()
        all_sent().wait_send()
        sent_in.wait_send()
        sent_out.wait_send()

    def relayed_chunk():
        all_forward.wait_recv()
        done = expert(direct_rows, far_rows)
        collected[extra(0), :] = done[:base]
        for k in reversed(range(1, half)):
            give_relay(k).start()

    groups = {
        "n0": range(0, plane),
        "n1": range(plane, half),
        "fa": range(half, half + plane),
        "fb": range(half + plane, n),
        "ff": range(half, n),
    }
    steps = {
        "pouch": send_pouch.start,
        "settle": settle,
        "most": lambda: gate(2),
        "all": lambda: gate(3),
        "relay": relay_out,
        "flags": send_flags,
        "relayed": relayed_chunk,
        "home": relay_home,
        "share": share_flags,
        "drain": drain,
    }
    for step in PLAN:
        if step in steps:
            steps[step]()
        elif step in groups:
            direct_chunk(groups[step])
        else:
            dispatch(step).start()

    arrived = jnp.zeros((tokens_here, width), jnp.float32)
    for name in FINISH:
        if name == "spill":
            swap_flag.wait_recv()
            worst = jnp.max(jnp.maximum(group_out[...], group_in[...]))
            spill_ref[0, 0] = worst.astype(jnp.int32)
            tell = pltpu.make_async_copy(spill_ref, spill_hbm, load_sem.at[0])
            tell.start()
            swap_flag.wait_send()
            continue
        if name == "pouch":
            here = pl.ds(direct_rows, spare)
            back_pouch.wait_recv()
        else:
            for group in sorted({slot // plane for slot in groups[name]}):
                came_back(group).wait_recv()
            here = rows_in_all(groups[name][0], groups[name][-1] + 1)
        arrived += jnp.dot(
            place[:, here], returned[here, :], preferred_element_type=jnp.float32
        )
    sums = tokens_ref[...].astype(jnp.float32) + columns[:, 1:2] * arrived
    out_ref[...] = sums.astype(jnp.bfloat16)

    back_pouch.wait_send()
    all_relay.wait_send()
    all_given().wait_send()
    tell.wait()


def with_relay(n, tokens, expert_ids, slot_ids, centroids, w_in, w_out):
    count, width = tokens.shape
    cap = 2 * count // n
    half = n // 2
    base = cap // 2
    spare = cap + cap // 2
    direct = half * (cap + base)
    hidden = w_in.shape[2]
    hbm = pl.BlockSpec(memory_space=pl.ANY)
    sems = pltpu.SemaphoreType.DMA
    flags = pltpu.SemaphoreType.REGULAR
    bf16 = jnp.bfloat16
    out, spill = pl.pallas_call(
        functools.partial(relay_kernel, n, cap, spare),
        out_shape=[
            pltpu.VMEM((count, width), bf16),
            jax.ShapeDtypeStruct((1, 1), jnp.int32),
        ],
        in_specs=[hbm] * 6,
        out_specs=[pl.BlockSpec(memory_space=pltpu.VMEM), hbm],
        scratch_shapes=[
            pltpu.VMEM((1, count), jnp.int32),
            pltpu.VMEM((1, count), jnp.int32),
            pltpu.VMEM((count, width), bf16),
            pltpu.VMEM(centroids.shape, bf16),
            pltpu.VMEM((direct, width), bf16),
            pltpu.VMEM((spare, width + 128), bf16),
            pltpu.VMEM((spare, width + 128), bf16),
            pltpu.VMEM((half * base, width), bf16),
            pltpu.VMEM((n * cap, width), bf16),
            pltpu.VMEM((n * cap, width), bf16),
            pltpu.VMEM((half * base, width), bf16),
            pltpu.VMEM((direct + spare, width), bf16),
            pltpu.VMEM((count, direct + spare), bf16),
            pltpu.VMEM((count, 128), jnp.float32),
            pltpu.VMEM((2, width, hidden), bf16),
            pltpu.VMEM((2, hidden, width), bf16),
            pltpu.VMEM((8, 128), jnp.float32),
            pltpu.VMEM((n, 8, 128), jnp.float32),
            pltpu.VMEM((8, 128), jnp.float32),
            pltpu.VMEM((8, 128), jnp.float32),
            pltpu.SMEM((1, 1), jnp.int32),
            sems((6,)),
            sems((2,)),
            sems((2, hidden // TILE)),
            sems((1,)),
            sems((4,)),
            sems((1,)),
            sems((4,)),
            sems((1,)),
            sems((1,)),
            sems((1,)),
            sems((1,)),
            sems((2,)),
            sems((2,)),
            sems((2,)),
            sems((2,)),
            flags((2,)),
            flags((4,)),
        ],
        compiler_params=pltpu.CompilerParams(
            collective_id=1, has_side_effects=True, vmem_limit_bytes=60 * 1024 * 1024
        ),
    )(
        expert_ids.reshape(1, count),
        slot_ids.reshape(1, count),
        tokens,
        centroids,
        w_in,
        w_out,
    )
    operands = (out, tokens, expert_ids, slot_ids, centroids, w_in, w_out)
    branches = (
        jax.make_jaxpr(lambda ready, *rest: ready)(*operands),
        jax.make_jaxpr(lambda ready, *rest: in_one_kernel(n, *rest))(*operands),
    )
    return cond_p.bind(spill[0, 0], *operands, branches=branches)[0]


def in_plain_ops(tokens, expert_ids, slot_ids, centroids, w_in, w_out):
    experts = centroids.shape[0]
    count_rows = tokens.shape[0]
    model_width = tokens.shape[1]
    capacity = 2 * count_rows // experts
    buffer_rows = expert_ids * capacity + slot_ids
    outgoing = (
        jnp.zeros((experts * capacity, model_width), jnp.bfloat16).at[buffer_rows].set(tokens)
    )
    outgoing = outgoing.reshape(experts, capacity, model_width)
    scores = jnp.dot(tokens, centroids.T, preferred_element_type=jnp.float32)
    columns = jnp.arange(experts, dtype=jnp.int32)
    chosen = jnp.sum(jnp.where(columns[None, :] == expert_ids[:, None], scores, 0.0), axis=1)
    gating = jax.nn.sigmoid(chosen)
    full_in, full_out = (
        lax.all_gather(w_in, "grp", axis=2, tiled=True),
        lax.all_gather(w_out, "grp", axis=1, tiled=True),
    )
    received = lax.all_to_all(outgoing, "ex", split_axis=0, concat_axis=0, tiled=True)
    flat_rows = received.reshape(-1, model_width)
    hidden = jnp.maximum(
        jnp.dot(flat_rows, full_in[0], preferred_element_type=jnp.float32), 0.0
    ).astype(jnp.bfloat16)
    result = jnp.dot(hidden, full_out[0], preferred_element_type=jnp.float32)
    returned = lax.all_to_all(
        result.astype(jnp.bfloat16).reshape(received.shape),
        "ex",
        split_axis=0,
        concat_axis=0,
        tiled=True,
    )
    arrived = returned.reshape(-1, model_width)[buffer_rows]
    mixed_rows = tokens.astype(jnp.float32) + gating[:, None] * arrived.astype(jnp.float32)
    return mixed_rows.astype(jnp.bfloat16)


def solution(mesh):
    n = mesh.shape["ex"]

    def on_device(tokens, expert_ids, slot_ids, centroids, w_in, w_out):
        capacity = 2 * tokens.shape[0] // n
        lanes_needed = (n // 2) * (capacity // 2)
        if mesh.shape["grp"] == 2 and n >= 8 and n & (n - 1) == 0 and capacity % 32 == 0 and lanes_needed <= 128:
            return with_relay(n, tokens, expert_ids, slot_ids, centroids, w_in, w_out)
        if mesh.shape["grp"] == 2 and n % 4 == 0 and capacity % 16 == 0:
            return in_one_kernel(n, tokens, expert_ids, slot_ids, centroids, w_in, w_out)
        return in_plain_ops(tokens, expert_ids, slot_ids, centroids, w_in, w_out)

    in_specs = (
        P(("grp", "ex"), None),
        P(("grp", "ex")),
        P(("grp", "ex")),
        P(),
        P("ex", None, "grp"),
        P("ex", "grp", None),
    )
    out_specs = P(("grp", "ex"), None)
    return jax.shard_map(
        on_device, mesh=mesh, in_specs=in_specs, out_specs=out_specs, check_vma=False
    )
```
